32 devices in a mesh: ep: 16 (over z, y, x), half: 2 (over core).
Axes of the slice: x: 2, y: 2, z: 4, core: 2. Of those that a mesh axis runs over, the one named last changes fastest.
Arguments:
- tokens: bfloat16 [2048, 2048], P('ep', 'half'), may hold values from -6 to 6
- gate_weights: float32 [2048, 8], P('ep'), may hold values from 0.05 to 0.3
- expert_ids: int32 [2048, 8], P('ep'), may hold values from 0 to 15, all different within a row; in each aligned block of 128 rows (0 to 127, 128 to 255, ...) at most 80 rows name the same one
- w_gate: bfloat16 [16, 2048, 768], P('ep', None, 'half'), may hold values from -0.125 to 0.125
- w_up: bfloat16 [16, 2048, 768], P('ep', None, 'half'), may hold values from -0.125 to 0.125
- w_down: bfloat16 [16, 768, 2048], P('ep', 'half'), may hold values from -0.21875 to 0.21875
Outputs:
- mixed: bfloat16 [2048, 2048], P('ep', 'half')
The draws below stay inside these ranges and needn't reach their ends.
Inputs may be any that keep to these rules, and one draw needn't show every extreme that they name: `expert_ids`: each row names 8 different experts. Within the rows of one device (aligned blocks of 128 rows) no expert is named by more than 80 rows, and in every draw some expert is named by exactly 80 rows of some block.
All inputs are finite; a program needn't handle non-finite values.
Results may differ from the reference program's by a relative error of at most 0.0085.
Values may be sent and summed in bfloat16 or wider, within the bound.
A program may use at most 64 MiB of HBM per device.

```python
import math
import jax
import jax.numpy as jnp
import numpy as np
from jax import lax

D = 2048
FF = 768
TOP = 8
TOK_DEV = 128
EXPERTS = 16
TOKENS = 2048
CAP = 80
N_EP = 16


def steps_of(own_key, shape, shards, low, largest):
    factor_of = 1.0
    for axis_at, shards_of in shards:
        steps = jax.random.uniform(jax.random.fold_in(jax.random.fold_in(own_key, 6), axis_at), (shards_of,), jnp.float32, low / len(shards), largest / len(shards))
        factor_of = factor_of * jnp.repeat(jnp.exp(steps), shape[axis_at] // shards_of).reshape((-1,) + (1,) * (len(shape) - 1 - axis_at))
    return factor_of


def deal_out(rng, own, number, rows, amount, top, reach, slope):
    sequence = jax.random.permutation(rng, amount)
    crowded, common = shares(amount, rows * top, reach, slope, True), shares(amount, rows * top, reach, slope, False)
    places = jnp.arange(amount)

    def named(lengths, rotation):
        used = int((lengths > 0).sum())
        fixed = max(1, used // 4)
        passed = fixed + (places - fixed + rotation * (used - fixed)) % max(1, amount - fixed)
        return jnp.zeros((amount,), jnp.int32).at[sequence[jnp.where(places < fixed, places, passed)]].set(jnp.asarray(lengths, jnp.int32))

    lengths = jnp.where(number % 4 == 0, named(crowded, number // 4), named(common, number - number // 4 - 1))
    mixed = jax.random.permutation(jax.random.fold_in(own, 3), amount)
    giver, receiver = mixed[0:amount // 2 * 2:2], mixed[1:amount // 2 * 2:2]
    margin = jnp.minimum(lengths[giver] - 1, reach - lengths[receiver]) // 2
    margin = jnp.where((giver == sequence[0]) | (receiver == sequence[0]) | (lengths[receiver] == 0), 0, jnp.maximum(margin, 0))
    passed = jax.random.randint(jax.random.fold_in(own, 4), (amount // 2,), 0, 1 << 20) % (margin + 1)
    lengths = lengths.at[giver].add(-passed).at[receiver].add(passed)
    items = jnp.searchsorted(jnp.cumsum(lengths), jnp.arange(rows * top), side="right").astype(jnp.int32)
    table = items.reshape(top, rows).T
    table = table[jax.random.permutation(jax.random.fold_in(own, 1), rows)]
    rotation = jax.random.randint(jax.random.fold_in(own, 2), (rows, 1), 0, top)
    return jnp.take_along_axis(table, (jnp.arange(top)[None, :] + rotation) % top, axis=1)


def shares(amount, total, limit, lean, full):
    weights = [(1 << 20) // math.isqrt(rank ** lean) + 1 for rank in range(1, amount + 1)]
    largest = limit if full else min(limit, max(-(-total // amount), total * weights[0] // sum(weights)))
    least = 1 if total - largest >= amount - 1 else 0
    holding, rest = [largest] + [least] * (amount - 1), total - largest - least * (amount - 1)
    while rest > 0:
        candidates = [i for i in range(1, amount) if holding[i] < largest] or [i for i in range(1, amount) if holding[i] < limit]
        pool, remaining = sum([weights[i] for i in candidates]), rest
        for i in candidates:
            more = min(limit - holding[i], max(1, remaining * weights[i] // pool), rest)
            holding[i] = holding[i] + more
            rest = rest - more
    return np.array(holding)


def scatter_about(key, extent, deviation, reach, shards=(), kind=jnp.bfloat16):
    entries = jax.random.normal(key, extent, jnp.float32) * deviation
    if len(shards) > 0:
        entries = steps_of(key, extent, shards, -0.22, 0.18) * entries
    return jnp.clip(entries, min=-reach, max=reach).astype(kind)


def setup_inputs(seed: int = 0) -> dict:
    arg_keys = jax.random.split(jax.random.key(seed), 7)
    tokens = scatter_about(arg_keys[0], (TOKENS, D), 1.0, 6.0, ((0, 16), (1, 2)))
    gate_weights = jnp.clip(0.05 + 0.25 * jax.random.uniform(arg_keys[1], (TOKENS, TOP), jnp.float32) ** steps_of(arg_keys[1], (TOKENS, TOP), ((0, 16),), -0.2, 0.2), 0.05, 0.3)
    expert_ids_keys = jax.random.split(jax.random.fold_in(arg_keys[2], 1), TOKENS // TOK_DEV)
    expert_ids_turns = jax.random.permutation(jax.random.fold_in(arg_keys[2], 3), TOKENS // TOK_DEV)
    expert_ids = jax.vmap(lambda own, number: deal_out(jax.random.fold_in(arg_keys[2], 2), own, number, TOK_DEV, EXPERTS, TOP, CAP, 2))(expert_ids_keys, expert_ids_turns).reshape((TOKENS, TOP))
    w_gate = scatter_about(arg_keys[3], (EXPERTS, D, FF), D ** -0.5, 0.125, ((0, 16), (2, 2)))
    w_up = scatter_about(arg_keys[4], (EXPERTS, D, FF), D ** -0.5, 0.125, ((0, 16), (2, 2)))
    w_down = scatter_about(arg_keys[5], (EXPERTS, FF, D), FF ** -0.5, 0.21875, ((0, 16), (1, 2)))
    return {"tokens": tokens, "gate_weights": gate_weights, "expert_ids": expert_ids, "w_gate": w_gate, "w_up": w_up, "w_down": w_down}


def rank_block(block):
    columns = jnp.arange(EXPERTS, dtype=jnp.int32)
    onehot = (block[:, None] == columns[None, :]).astype(jnp.int32)
    before = jnp.cumsum(onehot, axis=0) - onehot
    return jnp.sum(before * onehot, axis=1).astype(jnp.int32)


def reference(tokens, gate_weights, expert_ids, w_gate, w_up, w_down):
    ids = expert_ids.reshape(N_EP, TOK_DEV * TOP).astype(jnp.int32)
    ranks = lax.map(rank_block, ids)
    slot = (ids * CAP + ranks).astype(jnp.int32)
    source = jnp.arange(N_EP, dtype=jnp.int32)[:, None]
    local_token = (jnp.arange(TOK_DEV * TOP, dtype=jnp.int32) // TOP)[None, :]
    token_table = jnp.zeros((N_EP, EXPERTS * CAP), jnp.int32).at[source, slot].set(source * TOK_DEV + local_token)
    weight_table = jnp.zeros((N_EP, EXPERTS * CAP), jnp.float32).at[source, slot].set(gate_weights.reshape(N_EP, TOK_DEV * TOP))
    filled = jnp.zeros((N_EP, EXPERTS * CAP), jnp.bfloat16).at[source, slot].set(jnp.ones((N_EP, TOK_DEV * TOP), jnp.bfloat16))
    token_table = token_table.reshape(N_EP, EXPERTS, CAP).transpose(1, 0, 2).reshape(EXPERTS, N_EP * CAP)
    weight_table = weight_table.reshape(N_EP, EXPERTS, CAP).transpose(1, 0, 2).reshape(EXPERTS, N_EP * CAP)
    filled = filled.reshape(N_EP, EXPERTS, CAP).transpose(1, 0, 2).reshape(EXPERTS, N_EP * CAP)
    middle = FF // 2

    def expert_step(total, inputs):
        gate_mat, up_mat, down_mat, rows, weights, used = inputs
        slot_rows = tokens[rows] * used[:, None]
        gate = jnp.dot(slot_rows, gate_mat, preferred_element_type=jnp.float32)
        up = jnp.dot(slot_rows, up_mat, preferred_element_type=jnp.float32)
        hidden = (jax.nn.silu(gate) * up).astype(jnp.bfloat16)
        first = jnp.dot(hidden[:, :middle], down_mat[:middle], preferred_element_type=jnp.float32)
        second = jnp.dot(hidden[:, middle:], down_mat[middle:], preferred_element_type=jnp.float32)
        first = lax.optimization_barrier(first.astype(jnp.bfloat16)).astype(jnp.float32)
        second = lax.optimization_barrier(second.astype(jnp.bfloat16)).astype(jnp.float32)
        expert_out = lax.optimization_barrier((first + second).astype(jnp.bfloat16)).astype(jnp.float32)
        total = total.at[rows].add(weights[:, None] * expert_out)
        return total, None

    start = jnp.zeros((TOKENS, D), jnp.float32)
    total, unused = lax.scan(expert_step, start, (w_gate, w_up, w_down, token_table, weight_table, filled))
    return total.astype(jnp.bfloat16)
```

```python
import functools

import jax
import jax.numpy as jnp
from jax import lax
from jax.experimental import pallas as pl
from jax.experimental.pallas import tpu as pltpu
from jax.sharding import PartitionSpec as P

MESH = pl.DeviceIdType.MESH


def slot_count(tok_dev, top, experts):
    return min(tok_dev, max(2, 5 * tok_dev * top // (4 * experts)))


def slots(tokens, gate_weights, expert_ids, w_gate, w_up, w_down):
    tok_dev, half_width = tokens.shape
    top = expert_ids.shape[1]
    local_experts = w_gate.shape[0]
    experts = local_experts * lax.axis_size("ep")
    capacity = slot_count(tok_dev, top, experts)
    flat_ids = expert_ids.reshape(-1)
    columns = jnp.arange(experts, dtype=jnp.int32)
    onehot = (flat_ids[:, None] == columns[None, :]).astype(jnp.int32)
    ranks = jnp.sum((jnp.cumsum(onehot, axis=0) - onehot) * onehot, axis=1)
    slot = flat_ids * capacity + ranks
    token_of_pair = jnp.arange(tok_dev * top, dtype=jnp.int32) // top
    token_table = jnp.zeros((experts * capacity,), jnp.int32).at[slot].set(token_of_pair)
    filled = (
        jnp.zeros((experts * capacity,), jnp.bfloat16)
        .at[slot]
        .set(jnp.ones((tok_dev * top,), jnp.bfloat16))
    )
    outgoing = (tokens[token_table] * filled[:, None]).reshape(experts, capacity, half_width)
    received = lax.all_to_all(outgoing, "ep", split_axis=0, concat_axis=0, tiled=True)
    count = received.shape[1]
    whole = lax.all_gather(received, "half", axis=2, tiled=True)
    width = whole.shape[2]
    grouped = whole.reshape(-1, local_experts, count, width)
    gate = jnp.einsum("secd,edf->secf", grouped, w_gate, preferred_element_type=jnp.float32)
    up = jnp.einsum("secd,edf->secf", grouped, w_up, preferred_element_type=jnp.float32)
    hidden = (jax.nn.silu(gate) * up).astype(jnp.bfloat16)
    partial_out = jnp.einsum("secf,efd->secd", hidden, w_down, preferred_element_type=jnp.float32)
    partial_out = partial_out.astype(jnp.bfloat16).reshape(experts, count, width)
    widened = lax.optimization_barrier(partial_out).astype(jnp.float32)
    summed = lax.psum_scatter(widened.astype(jnp.bfloat16), "half", scatter_dimension=2, tiled=True)
    answer = lax.all_to_all(summed, "ep", split_axis=0, concat_axis=0, tiled=True)
    picked = answer.reshape(experts * capacity, -1)[slot].reshape(tok_dev, top, -1)
    slot_out = picked.astype(jnp.float32)
    mixed = jnp.einsum("tk,tkx->tx", gate_weights, slot_out)
    return mixed.astype(jnp.bfloat16)


def kernel(cap, tok_ref, gw_ref, ids_ref, wg_ref, wu_ref, wd_ref, out_ref,
           xo, xa, yb, rows_in, cx, cy, rx, ry, tab, wgu, wdn, po, pin, mine, res,
           rda, rdb, rcx, rcy, fx, fy, rfx, rfy, zs, zin, own, load_sem, ssem, rsem):
    ep = lax.axis_index("ep")
    core = lax.axis_index("half")
    x, y, z = ep % 2, (ep // 2) % 2, ep // 4
    tok, half = out_ref.shape
    part, ff = half // 2, wg_ref.shape[2]
    experts = tab.shape[2] // 2
    nz = tab.shape[0]
    f32, bf = jnp.float32, jnp.bfloat16
    inner = ((z + 1) // 2) % 2
    ex, ey = z * 4 + y * 2 + (1 - x), z * 4 + (1 - y) * 2 + x
    other, xn, yn = {"half": 1 - core}, {"ep": ex}, {"ep": ey}
    z1 = {"ep": (z + 1 - 2 * (z % 2)) * 4 + y * 2 + x}
    z3 = {"ep": (nz - 1 - z) * 4 + y * 2 + x}
    left, right = pl.ds(0, part), pl.ds(part, part)
    names = {}

    def send(name, src, dst, to):
        at = names.setdefault(name, len(names))
        return pltpu.make_async_remote_copy(
            src_ref=src, dst_ref=dst, send_sem=ssem.at[at], recv_sem=rsem.at[at],
            device_id=to, device_id_type=MESH,
        )

    sent = []

    def go(*args):
        copy = send(*args)
        copy.start()
        sent.append(copy)
        return copy

    h0, h1 = pl.ds(core * half, half), pl.ds((1 - core) * half, half)
    loads = []
    for at, (src, cols) in enumerate(((wg_ref, pl.ds(0, ff)), (wu_ref, pl.ds(ff, ff)))):
        for side, rows in enumerate((h0, h1)):
            loads.append(pltpu.make_async_copy(
                src.at[0, rows], wgu.at[pl.ds(side * half, half), cols], load_sem.at[2 * at + side]))
    for side, cols in enumerate((h0, h1)):
        cols = pl.ds(pl.multiple_of(cols.start, 128), half)
        loads.append(pltpu.make_async_copy(
            wd_ref.at[0, :, cols], wdn.at[:, pl.ds(side * half, half)], load_sem.at[4 + side]))
    for load in loads:
        load.start()

    expert_at = lax.broadcasted_iota(jnp.int32, (experts, tok), 0)
    chosen, weight = jnp.zeros((experts, tok), f32), jnp.zeros((experts, tok), f32)
    for k in range(ids_ref.shape[0]):
        hit = expert_at == ids_ref[k : k + 1, :]
        chosen += jnp.where(hit, 1.0, 0.0)
        weight += jnp.where(hit, gw_ref[k : k + 1, :], 0.0)
    before = lax.broadcasted_iota(jnp.int32, (tok, tok), 0) < lax.broadcasted_iota(jnp.int32, (tok, tok), 1)
    rank = jnp.dot(chosen.astype(bf), jnp.where(before, 1.0, 0.0).astype(bf), preferred_element_type=f32)
    tab[0, 0, 0:experts] = jnp.where(chosen > 0.0, rank, -1.0).astype(bf)
    tab[0, 0, experts : 2 * experts] = weight.astype(bf)

    barrier = pltpu.get_barrier_semaphore()
    for partner in (other, xn, yn, z1):
        pl.semaphore_signal(barrier, inc=1, device_id=partner, device_id_type=MESH)

    @pl.when(inner == 1)
    def _():
        pl.semaphore_signal(barrier, inc=1, device_id=z3, device_id_type=MESH)

    pl.semaphore_wait(barrier, 4 + inner)

    def block(d):
        return tok_ref if d == 0 else xo.at[d - 1]

    def piece(d, p):
        if p == 2:
            return tab.at[d, 0]
        return block(d).at[:, left if p == 0 else right]

    def along(d, p, came, to):
        return send(("z", d, p), piece(came, p), piece(d, p), to)

    order = (2, 0, 1)
    for p in order:
        along(1, p, 0, z1).start()

        @pl.when(inner == 1)
        def _():
            along(3, p, 0, z3).start()

        if p == 0:
            go(("xf", 0), piece(0, 0), xa.at[0], xn)
        if p == 1:
            go(("yf", 0), piece(0, 1), yb.at[0], yn)
        if p == 2:
            go(("xt", 0), tab.at[0, 0], tab.at[0, 1], xn)
            go(("yt", 0), tab.at[0, 0], tab.at[0, 2], yn)

    slot_at = lax.broadcasted_iota(jnp.int32, (cap, tok), 0).astype(f32)

    def row(d, line, e, base):
        table = tab[d, line, base : base + experts].astype(f32)
        return jnp.sum(jnp.where(expert_at == e, table, 0.0), axis=0, keepdims=True)

    def pick(d, line, es):
        parts = [jnp.where(slot_at == row(d, line, e, 0), 1.0, 0.0).astype(bf) for e in es]
        return jnp.concatenate(parts, axis=0)

    def spread(d, line, e, values):
        w = jnp.where(slot_at == row(d, line, e, 0), row(d, line, e, experts), 0.0)
        return lax.dot_general(w.astype(bf), values, (((0,), (0,)), ((), ())), preferred_element_type=f32)

    def waits(*copies):
        for copy in copies:
            copy.wait_recv()

    def expect(name, ref):
        send(name, ref, ref, other).wait_recv()

    def arrive(d):
        for p in order:
            if d == 3:
                @pl.when(inner == 0)
                def _():
                    expect(("z", 3, p), piece(3, p))
            else:
                expect(("z", d, p), piece(d, p))

            @pl.when(inner == 1)
            def _():
                if d == 1:
                    along(2, p, 1, z3).start()
                    expect(("z", 3, p), piece(3, p))
                    pltpu.make_async_remote_copy(
                        src_ref=piece(3, p), dst_ref=piece(2, p),
                        send_sem=ssem.at[names.setdefault(("z2", p), len(names))], recv_sem=rsem.at[names[("z", 2, p)]],
                        device_id=z1, device_id_type=MESH).start()
                if d == 2:
                    pltpu.make_async_remote_copy(
                        src_ref=piece(2, p), dst_ref=piece(3, p),
                        send_sem=ssem.at[names.setdefault(("z3", p), len(names))],
                        recv_sem=rsem.at[names[("z", 3, p)]],
                        device_id=z1, device_id_type=MESH).start()

            if p == 0:
                go(("xf", d), piece(d, 0), xa.at[d], xn)
            if p == 1:
                go(("yf", d), piece(d, 1), yb.at[d], yn)
            if p == 2:
                go(("xt", d), tab.at[d, 0], tab.at[d, 1], xn)
                go(("yt", d), tab.at[d, 0], tab.at[d, 2], yn)

    c1, c2, c3, c4 = (pl.ds(i * cap, cap) for i in range(4))
    lo, hi = pl.ds(0, half), pl.ds(half, half)

    def first(d):
        got = jnp.dot(pick(d, 0, (ep, ey)), block(d)[:, left], preferred_element_type=f32).astype(bf)
        rows_in[d, c1, left] = got[:cap]
        cy[d] = got[cap:]
        go(("yc", d), cy.at[d], rows_in.at[d, c3, left], yn)
        got = jnp.dot(pick(d, 0, (ep, ex)), block(d)[:, right], preferred_element_type=f32).astype(bf)
        rows_in[d, c1, right] = got[:cap]
        cx[d] = got[cap:]
        go(("xc", d), cx.at[d], rows_in.at[d, c2, right], xn)
        go(("g1", d), rows_in.at[d, c1, lo], rows_in.at[d, c1, hi], other)

    def second(d):
        expect(("xt", d), tab.at[d, 1])
        expect(("xf", d), xa.at[d])
        got = jnp.dot(pick(d, 1, (ep, ey)), xa[d], preferred_element_type=f32).astype(bf)
        rows_in[d, c2, left] = got[:cap]
        ry[d] = got[cap:]
        go(("yr", d), ry.at[d], rows_in.at[d, c4, left], yn)
        expect(("yt", d), tab.at[d, 2])
        expect(("yf", d), yb.at[d])
        got = jnp.dot(pick(d, 2, (ep, ex)), yb[d], preferred_element_type=f32).astype(bf)
        rows_in[d, c3, right] = got[:cap]
        rx[d] = got[cap:]
        go(("xr", d), rx.at[d], rows_in.at[d, c4, right], xn)

    mid = pl.ds(cap, 2 * cap)

    def third(d):
        expect(("xc", d), rows_in.at[d, c2, right])
        expect(("yc", d), rows_in.at[d, c3, left])
        go(("g2", d), rows_in.at[d, mid, lo], rows_in.at[d, mid, hi], other)
        expect(("yr", d), rows_in.at[d, c4, left])
        expect(("xr", d), rows_in.at[d, c4, right])
        go(("g3", d), rows_in.at[d, c4, lo], rows_in.at[d, c4, hi], other)

    def compute(d):
        expect(("g1", d), rows_in.at[d, c1, hi])
        expect(("g2", d), rows_in.at[d, mid, hi])
        expect(("g3", d), rows_in.at[d, c4, hi])
        gu = jnp.dot(rows_in[d], wgu[...], preferred_element_type=f32)
        gate, up = gu[:, :ff], gu[:, ff:]
        hidden = (gate / (1.0 + jnp.exp(-gate)) * up).astype(bf)
        po[d] = jnp.dot(hidden, wdn[:, half:], preferred_element_type=f32).astype(bf)
        go(("p", d), po.at[d], pin.at[d], other)
        mine[d] = jnp.dot(hidden, wdn[:, :half], preferred_element_type=f32).astype(bf)

    def close(d):
        expect(("p", d), pin.at[d])
        res[d] = (mine[d].astype(f32) + pin[d].astype(f32)).astype(bf)
        go(("da", d), res.at[d, c4, left], rda.at[d], yn)
        go(("db", d), res.at[d, c4, right], rdb.at[d], xn)
        go(("cy", d), res.at[d, c3, left], rcy.at[d], yn)
        go(("cx", d), res.at[d, c2, right], rcx.at[d], xn)

    def relay(d):
        expect(("da", d), rda.at[d])
        fx[d] = (spread(d, 1, ep, res[d, c2, left]) + spread(d, 1, ey, rda[d])).astype(bf)
        go(("fx", d), fx.at[d], rfx.at[d], xn)
        expect(("db", d), rdb.at[d])
        fy[d] = (spread(d, 2, ep, res[d, c3, right]) + spread(d, 2, ex, rdb[d])).astype(bf)
        go(("fy", d), fy.at[d], rfy.at[d], yn)

    def home(d):
        expect(("cy", d), rcy.at[d])
        expect(("fx", d), rfx.at[d])
        a = spread(d, 0, ep, res[d, c1, left]) + spread(d, 0, ey, rcy[d]) + rfx[d].astype(f32)
        expect(("cx", d), rcx.at[d])
        expect(("fy", d), rfy.at[d])
        b = spread(d, 0, ep, res[d, c1, right]) + spread(d, 0, ex, rcx[d]) + rfy[d].astype(f32)
        if d:
            zs[d - 1, :, left] = a.astype(bf)
            zs[d - 1, :, right] = b.astype(bf)

            @pl.when(inner == 0)
            def _():
                send(("s", d), zs.at[d - 1], zin.at[d - 1], z1).start()
        else:
            own[:, left] = a
            own[:, right] = b

    def link(got, add, name, to, slot):
        expect(got, zin.at[0])
        at = got[1] - 1
        zs[add - 1] = (zs[add - 1].astype(f32) + zin[at].astype(f32)).astype(bf)
        send(name, zs.at[add - 1], zin.at[slot], to).start()

    arrive0 = [first, second]
    for stage in arrive0:
        stage(0)
    arrive(1)
    first(1)
    third(0)
    second(1)
    for load in loads:
        load.wait()
    compute(0)
    arrive(2)
    first(2)
    third(1)
    second(2)
    compute(1)
    arrive(3)
    first(3)
    third(2)
    second(3)
    compute(2)
    close(2)
    close(1)
    third(3)
    compute(3)
    close(3)
    relay(2)
    relay(3)
    close(0)
    relay(1)
    home(2)
    home(3)

    @pl.when(inner == 1)
    def _():
        link(("s", 2), 3, ("s", 4), z3, 3)
        link(("s", 3), 2, ("s", 5), z3, 4)

    relay(0)
    home(1)

    @pl.when(inner == 1)
    def _():
        link(("s", 5), 1, ("s", 6), z1, 5)

    home(0)

    @pl.when(inner == 1)
    def _():
        expect(("s", 1), zin.at[0])
        expect(("s", 4), zin.at[3])
        total = own[...] + zin[0].astype(f32) + zin[3].astype(f32)
        out_ref[...] = total.astype(bf)
        for copy in (
            [send(("z", 3, p), piece(0, p), piece(3, p), z3) for p in order]
            + [send(("z", 2, p), piece(1, p), piece(2, p), z3) for p in order]
            + [send(("z2", p), piece(3, p), piece(2, p), z1) for p in order]
            + [send(("z3", p), piece(2, p), piece(3, p), z1) for p in order]
            + [send(("s", 4 + i), zs.at[0], zin.at[0], z3) for i in range(3)]
        ):
            copy.wait_send()

    @pl.when(inner == 0)
    def _():
        expect(("s", 6), zin.at[5])
        out_ref[...] = (own[...] + zin[5].astype(f32)).astype(bf)
        for d in range(1, nz):
            send(("s", d), zs.at[d - 1], zin.at[d - 1], z1).wait_send()

    for p in order:
        along(1, p, 0, z1).wait_send()
    for copy in sent:
        copy.wait_send()


def multicast(tokens, gate_weights, expert_ids, w_gate, w_up, w_down):
    tok, half = tokens.shape
    experts = w_gate.shape[0] * lax.axis_size("ep")
    nz = lax.axis_size("ep") // 4
    part, width, ff = half // 2, w_gate.shape[1], w_gate.shape[2]
    cap = slot_count(tok, expert_ids.shape[1], experts)
    bf, dma = jnp.bfloat16, pltpu.SemaphoreType.DMA
    vmem, hbm = pl.BlockSpec(memory_space=pltpu.VMEM), pl.BlockSpec(memory_space=pl.ANY)
    compact, full = pltpu.VMEM((nz, cap, part), bf), pltpu.VMEM((nz, tok, part), bf)
    wide = pltpu.VMEM((nz, 4 * cap, half), bf)
    return pl.pallas_call(
        functools.partial(kernel, cap),
        out_shape=jax.ShapeDtypeStruct((tok, half), bf),
        in_specs=[vmem, vmem, vmem, hbm, hbm, hbm],
        out_specs=vmem,
        scratch_shapes=[
            pltpu.VMEM((nz - 1, tok, half), bf), full, full,
            pltpu.VMEM((nz, 4 * cap, width), bf),
            compact, compact, compact, compact,
            pltpu.VMEM((nz, 3, 2 * experts, tok), bf),
            pltpu.VMEM((width, 2 * ff), bf),
            pltpu.VMEM((ff, width), bf),
            wide, wide, wide, wide,
            compact, compact, compact, compact,
            full, full, full, full,
            pltpu.VMEM((nz - 1, tok, half), bf),
            pltpu.VMEM((6, tok, half), bf),
            pltpu.VMEM((tok, half), jnp.float32),
            dma((6,)), dma((104,)), dma((104,)),
        ],
        compiler_params=pltpu.CompilerParams(
            collective_id=0, has_side_effects=True, vmem_limit_bytes=60 * 1024 * 1024
        ),
    )(tokens, gate_weights.T, expert_ids.T, w_gate, w_up, w_down)


def local(tokens, gate_weights, expert_ids, w_gate, w_up, w_down):
    tok_dev, half = tokens.shape
    devices, cores = lax.axis_size("ep"), lax.axis_size("half")
    experts = w_gate.shape[0] * devices
    cap = slot_count(tok_dev, expert_ids.shape[1], experts)
    fits = tok_dev * devices * half * 2 <= 8 * 1024 * 1024 and w_gate.shape[0] == 1
    shaped = cores == 2 and devices == 4 * 4 and tok_dev == 128
    tiled = cap % 16 == 0 and half % 256 == 0 and experts % 16 == 0 and w_gate.shape[2] % 128 == 0
    plan = multicast if fits and shaped and tiled else slots
    return plan(tokens, gate_weights, expert_ids, w_gate, w_up, w_down)


def solution(mesh):
    placed = (
        P("ep", "half"),
        P("ep", None),
        P("ep", None),
        P("ep", None, "half"),
        P("ep", None, "half"),
        P("ep", "half", None),
    )
    return jax.shard_map(
        local, mesh=mesh, in_specs=placed, out_specs=P("ep", "half"), check_vma=False
    )
```

```python
import functools

import jax
import jax.numpy as jnp
from jax import lax
from jax.experimental import pallas as pl
from jax.experimental.pallas import tpu as pltpu
from jax.sharding import PartitionSpec as P

MESH = pl.DeviceIdType.MESH


def slot_count(tok_dev, top, experts):
    return min(tok_dev, max(2, 5 * tok_dev * top // (4 * experts)))


def slots(tokens, gate_weights, expert_ids, w_gate, w_up, w_down):
    tok_dev, half_width = tokens.shape
    top = expert_ids.shape[1]
    local_experts = w_gate.shape[0]
    experts = local_experts * lax.axis_size("ep")
    capacity = slot_count(tok_dev, top, experts)
    flat_ids = expert_ids.reshape(-1)
    columns = jnp.arange(experts, dtype=jnp.int32)
    onehot = (flat_ids[:, None] == columns[None, :]).astype(jnp.int32)
    ranks = jnp.sum((jnp.cumsum(onehot, axis=0) - onehot) * onehot, axis=1)
    slot = flat_ids * capacity + ranks
    token_of_pair = jnp.arange(tok_dev * top, dtype=jnp.int32) // top
    token_table = jnp.zeros((experts * capacity,), jnp.int32).at[slot].set(token_of_pair)
    filled = (
        jnp.zeros((experts * capacity,), jnp.bfloat16)
        .at[slot]
        .set(jnp.ones((tok_dev * top,), jnp.bfloat16))
    )
    outgoing = (tokens[token_table] * filled[:, None]).reshape(experts, capacity, half_width)
    received = lax.all_to_all(outgoing, "ep", split_axis=0, concat_axis=0, tiled=True)
    count = received.shape[1]
    whole = lax.all_gather(received, "half", axis=2, tiled=True)
    width = whole.shape[2]
    grouped = whole.reshape(-1, local_experts, count, width)
    gate = jnp.einsum("secd,edf->secf", grouped, w_gate, preferred_element_type=jnp.float32)
    up = jnp.einsum("secd,edf->secf", grouped, w_up, preferred_element_type=jnp.float32)
    hidden = (jax.nn.silu(gate) * up).astype(jnp.bfloat16)
    partial_out = jnp.einsum("secf,efd->secd", hidden, w_down, preferred_element_type=jnp.float32)
    partial_out = partial_out.astype(jnp.bfloat16).reshape(experts, count, width)
    widened = lax.optimization_barrier(partial_out).astype(jnp.float32)
    summed = lax.psum_scatter(widened.astype(jnp.bfloat16), "half", scatter_dimension=2, tiled=True)
    answer = lax.all_to_all(summed, "ep", split_axis=0, concat_axis=0, tiled=True)
    picked = answer.reshape(experts * capacity, -1)[slot].reshape(tok_dev, top, -1)
    slot_out = picked.astype(jnp.float32)
    mixed = jnp.einsum("tk,tkx->tx", gate_weights, slot_out)
    return mixed.astype(jnp.bfloat16)


PLANS = (
    "F0 A12 A10 S0 A11 F1 A22 A20 T0 S1 W C0 A21 F2 A32 T1 A30 S2 A31 F3 C1 K0 T2 S3 C2 K1"
    " T3 K2 R1 C3 R2 H1 K3 H2 R3 R0 H3 H0",
    "F0 A12 A22 A10 A20 S0 A11 A21 F1 F2 A32 A30 T0 S1 A31 F3 W C0 S2 T1 C1 K0 T2 S3 C2 K1"
    " T3 K2 R1 C3 R2 H1 K3 H2 R3 R0 H3 H0",
)


def kernel(cap, tok_ref, gw_ref, ids_ref, wg_ref, wu_ref, wd_ref, out_ref,
           xo, xa, yb, rows_in, cx, cy, rx, ry, tab, wgu, wdn, po, pin, mine, res,
           rda, rdb, rcx, rcy, fx, fy, rfx, rfy, zs, zin, own, load_sem, ssem, rsem):
    ep = lax.axis_index("ep")
    core = lax.axis_index("half")
    x, y, z = ep % 2, (ep // 2) % 2, ep // 4
    tok, half = out_ref.shape
    part, rows, ff = half // 2, tok // 2, wg_ref.shape[2]
    experts = tab.shape[2] // 2
    nz = tab.shape[0]
    f32, bf = jnp.float32, jnp.bfloat16
    inner = ((z + 1) // 2) % 2
    ex, ey = z * 4 + y * 2 + (1 - x), z * 4 + (1 - y) * 2 + x
    other, xn, yn = {"half": 1 - core}, {"ep": ex}, {"ep": ey}
    z1 = {"ep": (z + 1 - 2 * (z % 2)) * 4 + y * 2 + x}
    z3 = {"ep": (nz - 1 - z) * 4 + y * 2 + x}
    left, right = pl.ds(0, part), pl.ds(part, part)
    names = {}

    def send(name, src, dst, to, lands=None):
        at = names.setdefault(name, len(names))
        got = at if lands is None else names.setdefault(lands, len(names))
        return pltpu.make_async_remote_copy(
            src_ref=src, dst_ref=dst, send_sem=ssem.at[at], recv_sem=rsem.at[got],
            device_id=to, device_id_type=MESH,
        )

    sent = []

    def move(copy):
        copy.start()
        sent.append(copy)

    def go(*args):
        move(send(*args))

    h0, h1 = pl.ds(core * half, half), pl.ds((1 - core) * half, half)
    loads = []
    for at, (src, cols) in enumerate(((wg_ref, pl.ds(0, ff)), (wu_ref, pl.ds(ff, ff)))):
        for side, deep in enumerate((h0, h1)):
            loads.append(pltpu.make_async_copy(
                src.at[0, deep], wgu.at[pl.ds(side * half, half), cols], load_sem.at[2 * at + side]))
    for side, cols in enumerate((h0, h1)):
        cols = pl.ds(pl.multiple_of(cols.start, 128), half)
        loads.append(pltpu.make_async_copy(
            wd_ref.at[0, :, cols], wdn.at[:, pl.ds(side * half, half)], load_sem.at[4 + side]))
    for load in loads:
        load.start()

    expert_at = lax.broadcasted_iota(jnp.int32, (experts, tok), 0)
    chosen, weight = jnp.zeros((experts, tok), f32), jnp.zeros((experts, tok), f32)
    for k in range(ids_ref.shape[0]):
        hit = expert_at == ids_ref[k : k + 1, :]
        chosen += jnp.where(hit, 1.0, 0.0)
        weight += jnp.where(hit, gw_ref[k : k + 1, :], 0.0)
    before = lax.broadcasted_iota(jnp.int32, (tok, tok), 0) < lax.broadcasted_iota(jnp.int32, (tok, tok), 1)
    rank = jnp.dot(chosen.astype(bf), jnp.where(before, 1.0, 0.0).astype(bf), preferred_element_type=f32)
    tab[0, 0, 0:experts] = jnp.where(chosen > 0.0, rank, -1.0).astype(bf)
    tab[0, 0, experts : 2 * experts] = weight.astype(bf)

    barrier = pltpu.get_barrier_semaphore()
    for partner in (other, xn, yn, z1):
        pl.semaphore_signal(barrier, inc=1, device_id=partner, device_id_type=MESH)

    @pl.when(inner == 1)
    def _():
        pl.semaphore_signal(barrier, inc=1, device_id=z3, device_id_type=MESH)

    pl.semaphore_wait(barrier, 4 + inner)

    def block(d):
        return tok_ref if d == 0 else xo.at[d - 1]

    def piece(d, p):
        return tab.at[d, 0] if p == 2 else block(d).at[pl.ds(p * rows, rows)]

    def hop(name, lands, p, came, to):
        return send((name, p), piece(came, p), piece(lands, p), to, ("z", lands, p))

    def plane(d, p):
        if p == 2:
            go(("xt", d), tab.at[d, 0], tab.at[d, 1], xn)
            go(("yt", d), tab.at[d, 0], tab.at[d, 2], yn)
        else:
            here = pl.ds(p * rows, rows)
            go(("xf", d, p), block(d).at[here, left], xa.at[d, here], xn)
            go(("yf", d, p), block(d).at[here, right], yb.at[d, here], yn)

    order = (2, 0, 1)

    def begin(role):
        for p in order:
            move(hop("z own", 1 if role else 2, p, 0, z1))
            if role:
                move(hop("z far", 1, p, 0, z3))
            plane(0, p)

    slot_at = lax.broadcasted_iota(jnp.int32, (cap, tok), 0).astype(f32)

    def row(d, line, e, base):
        table = tab[d, line, base : base + experts].astype(f32)
        return jnp.sum(jnp.where(expert_at == e, table, 0.0), axis=0, keepdims=True)

    def pick(d, line, es):
        parts = [jnp.where(slot_at == row(d, line, e, 0), 1.0, 0.0).astype(bf) for e in es]
        return jnp.concatenate(parts, axis=0)

    def spread(d, line, e, values):
        w = jnp.where(slot_at == row(d, line, e, 0), row(d, line, e, experts), 0.0)
        return lax.dot_general(w.astype(bf), values, (((0,), (0,)), ((), ())), preferred_element_type=f32)

    def expect(name, ref):
        send(name, ref, ref, other).wait_recv()

    def arrive(role, d, p):
        expect(("z", d, p), piece(d, p))
        if role:
            lands, to = ((2, z1), (3, z3), (3, z1))[d - 1]
            move(hop("z on" + str(d), lands, p, d, to))
        plane(d, p)

    c1, c2, c3, c4 = (pl.ds(i * cap, cap) for i in range(4))
    lo, hi = pl.ds(0, half), pl.ds(half, half)

    def first(d):
        got = jnp.dot(pick(d, 0, (ep, ey)), block(d)[:, left], preferred_element_type=f32).astype(bf)
        rows_in[d, c1, left] = got[:cap]
        cy[d] = got[cap:]
        go(("yc", d), cy.at[d], rows_in.at[d, c3, left], yn)
        got = jnp.dot(pick(d, 0, (ep, ex)), block(d)[:, right], preferred_element_type=f32).astype(bf)
        rows_in[d, c1, right] = got[:cap]
        cx[d] = got[cap:]
        go(("xc", d), cx.at[d], rows_in.at[d, c2, right], xn)
        go(("g1", d), rows_in.at[d, c1, lo], rows_in.at[d, c1, hi], other)

    def second(d):
        expect(("xt", d), tab.at[d, 1])
        for p in range(2):
            expect(("xf", d, p), xa.at[d, pl.ds(p * rows, rows)])
        got = jnp.dot(pick(d, 1, (ep, ey)), xa[d], preferred_element_type=f32).astype(bf)
        rows_in[d, c2, left] = got[:cap]
        ry[d] = got[cap:]
        go(("yr", d), ry.at[d], rows_in.at[d, c4, left], yn)
        expect(("yt", d), tab.at[d, 2])
        for p in range(2):
            expect(("yf", d, p), yb.at[d, pl.ds(p * rows, rows)])
        got = jnp.dot(pick(d, 2, (ep, ex)), yb[d], preferred_element_type=f32).astype(bf)
        rows_in[d, c3, right] = got[:cap]
        rx[d] = got[cap:]
        go(("xr", d), rx.at[d], rows_in.at[d, c4, right], xn)

    mid = pl.ds(cap, 2 * cap)

    def third(d):
        expect(("xc", d), rows_in.at[d, c2, right])
        expect(("yc", d), rows_in.at[d, c3, left])
        go(("g2", d), rows_in.at[d, mid, lo], rows_in.at[d, mid, hi], other)
        expect(("yr", d), rows_in.at[d, c4, left])
        expect(("xr", d), rows_in.at[d, c4, right])
        go(("g3", d), rows_in.at[d, c4, lo], rows_in.at[d, c4, hi], other)

    def compute(d):
        expect(("g1", d), rows_in.at[d, c1, hi])
        expect(("g2", d), rows_in.at[d, mid, hi])
        expect(("g3", d), rows_in.at[d, c4, hi])
        gu = jnp.dot(rows_in[d], wgu[...], preferred_element_type=f32)
        gate, up = gu[:, :ff], gu[:, ff:]
        hidden = (gate / (1.0 + jnp.exp(-gate)) * up).astype(bf)
        po[d] = jnp.dot(hidden, wdn[:, half:], preferred_element_type=f32).astype(bf)
        go(("p", d), po.at[d], pin.at[d], other)
        mine[d] = jnp.dot(hidden, wdn[:, :half], preferred_element_type=f32).astype(bf)

    def close(d):
        expect(("p", d), pin.at[d])
        res[d] = (mine[d].astype(f32) + pin[d].astype(f32)).astype(bf)
        go(("da", d), res.at[d, c4, left], rda.at[d], yn)
        go(("db", d), res.at[d, c4, right], rdb.at[d], xn)
        go(("cy", d), res.at[d, c3, left], rcy.at[d], yn)
        go(("cx", d), res.at[d, c2, right], rcx.at[d], xn)

    def relay(d):
        expect(("da", d), rda.at[d])
        fx[d] = (spread(d, 1, ep, res[d, c2, left]) + spread(d, 1, ey, rda[d])).astype(bf)
        go(("fx", d), fx.at[d], rfx.at[d], xn)
        expect(("db", d), rdb.at[d])
        fy[d] = (spread(d, 2, ep, res[d, c3, right]) + spread(d, 2, ex, rdb[d])).astype(bf)
        go(("fy", d), fy.at[d], rfy.at[d], yn)

    apart = (z + 1 - 2 * (z % 2), (z + 2) % nz, nz - 1 - z)
    def home(role, d):
        for p, cols in enumerate((left, right)):
            e, part_in, full = (ey, rcy, rfx) if p == 0 else (ex, rcx, rfy)
            expect(("cy" if p == 0 else "cx", d), part_in.at[d])
            expect(("fx" if p == 0 else "fy", d), full.at[d])
            total = spread(d, 0, ep, res[d, c1, cols]) + spread(d, 0, e, part_in[d]) + full[d].astype(f32)
            if d == 0:
                own[:, cols] = total
                continue
            zs[d - 1, :, cols] = total.astype(bf)
            step = (d + 1) % 3 if role else d - 1
            go(("o", d, p), zs.at[d - 1, :, cols], zin.at[step, :, cols],
               {"ep": apart[step] * 4 + y * 2 + x}, ("s", step, p))

    def ready(_):
        for load in loads:
            load.wait()

    def finish(_):
        for p, cols in enumerate((left, right)):
            total = own[:, cols]
            for d in range(nz - 1):
                expect(("s", d, p), zin.at[d, :, cols])
                total += zin[d, :, cols].astype(f32)
            out_ref[:, cols] = total.astype(bf)
        for copy in sent:
            copy.wait_send()
        sent.clear()

    steps = {"F": first, "S": second, "T": third, "C": compute, "K": close, "R": relay}
    for role, plan in enumerate(PLANS):
        @pl.when(inner == role)
        def _():
            begin(role)
            for word in plan.split():
                at = [int(v) for v in word[1:]]
                if word[0] in "AH":
                    {"A": arrive, "H": home}[word[0]](role, *at)
                elif word[0] == "W":
                    ready(at)
                else:
                    steps[word[0]](*at)
            finish(role)


def multicast(tokens, gate_weights, expert_ids, w_gate, w_up, w_down):
    tok, half = tokens.shape
    experts = w_gate.shape[0] * lax.axis_size("ep")
    nz = lax.axis_size("ep") // 4
    part, width, ff = half // 2, w_gate.shape[1], w_gate.shape[2]
    cap = slot_count(tok, expert_ids.shape[1], experts)
    bf, dma = jnp.bfloat16, pltpu.SemaphoreType.DMA
    vmem, hbm = pl.BlockSpec(memory_space=pltpu.VMEM), pl.BlockSpec(memory_space=pl.ANY)
    compact, full = pltpu.VMEM((nz, cap, part), bf), pltpu.VMEM((nz, tok, part), bf)
    wide = pltpu.VMEM((nz, 4 * cap, half), bf)
    return pl.pallas_call(
        functools.partial(kernel, cap),
        out_shape=jax.ShapeDtypeStruct((tok, half), bf),
        in_specs=[vmem, vmem, vmem, hbm, hbm, hbm],
        out_specs=vmem,
        scratch_shapes=[
            pltpu.VMEM((nz - 1, tok, half), bf), full, full,
            pltpu.VMEM((nz, 4 * cap, width), bf),
            compact, compact, compact, compact,
            pltpu.VMEM((nz, 3, 2 * experts, tok), bf),
            pltpu.VMEM((width, 2 * ff), bf),
            pltpu.VMEM((ff, width), bf),
            wide, wide, wide, wide,
            compact, compact, compact, compact,
            full, full, full, full,
            pltpu.VMEM((nz - 1, tok, half), bf),
            pltpu.VMEM((nz - 1, tok, half), bf),
            pltpu.VMEM((tok, half), jnp.float32),
            dma((6,)), dma((136,)), dma((136,)),
        ],
        compiler_params=pltpu.CompilerParams(
            collective_id=0, has_side_effects=True, vmem_limit_bytes=60 * 1024 * 1024
        ),
    )(tokens, gate_weights.T, expert_ids.T, w_gate, w_up, w_down)


def local(tokens, gate_weights, expert_ids, w_gate, w_up, w_down):
    tok_dev, half = tokens.shape
    devices, cores = lax.axis_size("ep"), lax.axis_size("half")
    experts = w_gate.shape[0] * devices
    cap = slot_count(tok_dev, expert_ids.shape[1], experts)
    fits = tok_dev * devices * half * 2 <= 8 * 1024 * 1024 and w_gate.shape[0] == 1
    shaped = cores == 2 and devices == 4 * 4 and tok_dev == 128
    tiled = cap % 16 == 0 and half % 256 == 0 and experts % 16 == 0 and w_gate.shape[2] % 128 == 0
    plan = multicast if fits and shaped and tiled else slots
    return plan(tokens, gate_weights, expert_ids, w_gate, w_up, w_down)


def solution(mesh):
    placed = (
        P("ep", "half"),
        P("ep", None),
        P("ep", None),
        P("ep", None, "half"),
        P("ep", None, "half"),
        P("ep", "half", None),
    )
    return jax.shard_map(
        local, mesh=mesh, in_specs=placed, out_specs=P("ep", "half"), check_vma=False
    )
```

```python
import functools

import jax
import jax.numpy as jnp
from jax import lax
from jax.experimental import pallas as pl
from jax.experimental.pallas import tpu as pltpu
from jax.sharding import PartitionSpec as P

MESH = pl.DeviceIdType.MESH


def slot_count(tok_dev, top, experts):
    return min(tok_dev, max(2, 5 * tok_dev * top // (4 * experts)))


def slots(tokens, gate_weights, expert_ids, w_gate, w_up, w_down):
    tok_dev, half_width = tokens.shape
    top = expert_ids.shape[1]
    local_experts = w_gate.shape[0]
    experts = local_experts * lax.axis_size("ep")
    capacity = slot_count(tok_dev, top, experts)
    flat_ids = expert_ids.reshape(-1)
    columns = jnp.arange(experts, dtype=jnp.int32)
    onehot = (flat_ids[:, None] == columns[None, :]).astype(jnp.int32)
    ranks = jnp.sum((jnp.cumsum(onehot, axis=0) - onehot) * onehot, axis=1)
    slot = flat_ids * capacity + ranks
    token_of_pair = jnp.arange(tok_dev * top, dtype=jnp.int32) // top
    token_table = jnp.zeros((experts * capacity,), jnp.int32).at[slot].set(token_of_pair)
    filled = (
        jnp.zeros((experts * capacity,), jnp.bfloat16)
        .at[slot]
        .set(jnp.ones((tok_dev * top,), jnp.bfloat16))
    )
    outgoing = (tokens[token_table] * filled[:, None]).reshape(experts, capacity, half_width)
    received = lax.all_to_all(outgoing, "ep", split_axis=0, concat_axis=0, tiled=True)
    count = received.shape[1]
    whole = lax.all_gather(received, "half", axis=2, tiled=True)
    width = whole.shape[2]
    grouped = whole.reshape(-1, local_experts, count, width)
    gate = jnp.einsum("secd,edf->secf", grouped, w_gate, preferred_element_type=jnp.float32)
    up = jnp.einsum("secd,edf->secf", grouped, w_up, preferred_element_type=jnp.float32)
    hidden = (jax.nn.silu(gate) * up).astype(jnp.bfloat16)
    partial_out = jnp.einsum("secf,efd->secd", hidden, w_down, preferred_element_type=jnp.float32)
    partial_out = partial_out.astype(jnp.bfloat16).reshape(experts, count, width)
    widened = lax.optimization_barrier(partial_out).astype(jnp.float32)
    summed = lax.psum_scatter(widened.astype(jnp.bfloat16), "half", scatter_dimension=2, tiled=True)
    answer = lax.all_to_all(summed, "ep", split_axis=0, concat_axis=0, tiled=True)
    picked = answer.reshape(experts * capacity, -1)[slot].reshape(tok_dev, top, -1)
    slot_out = picked.astype(jnp.float32)
    mixed = jnp.einsum("tk,tkx->tx", gate_weights, slot_out)
    return mixed.astype(jnp.bfloat16)


PLANS = (
    (
        "A12", "X0", "F0", "A10", "W", "A11", "A22", "F1", "X1", "A20", "Y1", "T1", "A21", "A32",
        "A30", "U1", "A31", "F3", "C1", "X3", "Y3", "K1", "X2", "Y2", "F2", "Y0", "T3", "U3", "L1",
        "C3", "U2", "Q1", "T2", "T0", "K3", "R1", "L3", "C2", "J1", "Q3", "K2", "U0", "H1", "R3",
        "C0", "Q2", "L2", "J3", "R2", "H3", "J2", "K0", "L0", "H2", "R0", "Q0", "H0", "J0",
    ),
    (
        "A22", "F0", "A12", "A10", "A20", "A21", "A32", "A11", "A30", "F1", "Y1", "X1", "A31", "F3",
        "T1", "X2", "U1", "Y2", "Y3", "X3", "X0", "W", "C1", "T3", "F2", "K1", "L1", "U3", "Y0",
        "C3", "Q1", "T2", "U2", "K3", "R1", "C2", "J1", "Q3", "L3", "R3", "T0", "H1", "K2", "J3",
        "H3", "Q2", "R2", "L2", "U0", "C0", "K0", "J2", "L0", "R0", "Q0", "H2", "H0", "J0",
    ),
)


def kernel(cap, *refs):
    dma = pltpu.SemaphoreType.DMA
    pl.run_scoped(functools.partial(body, cap, *refs), dma((12,)), dma((136,)), dma((136,)))


def body(cap, tok_hbm, gw_hbm, ids_hbm, wg_ref, wu_ref, wd_ref, out_ref,
         tok_ref, gw_ref, ids_ref, xo, xa, yb, rows_in, cx, cy, rx, ry, tab, wgu, wdn, po, pin, mine, res,
         rda, rdb, rcx, rcy, fx, fy, rfx, rfy, zs, zin, own, load_sem, ssem, rsem):
    ep = lax.axis_index("ep")
    core = lax.axis_index("half")
    x, y, z = ep % 2, (ep // 2) % 2, ep // 4
    tok, half = out_ref.shape
    part, rows, ff = half // 2, tok // 2, wg_ref.shape[2]
    experts = tab.shape[2] // 2
    nz = tab.shape[0]
    f32, bf = jnp.float32, jnp.bfloat16
    inner = ((z + 1) // 2) % 2
    ex, ey = z * 4 + y * 2 + (1 - x), z * 4 + (1 - y) * 2 + x
    other, xn, yn = {"half": 1 - core}, {"ep": ex}, {"ep": ey}
    z1 = {"ep": (z + 1 - 2 * (z % 2)) * 4 + y * 2 + x}
    z3 = {"ep": (nz - 1 - z) * 4 + y * 2 + x}
    left, right = pl.ds(0, part), pl.ds(part, part)
    names = {}

    def send(name, src, dst, to, lands=None):
        at = names.setdefault(name, len(names))
        got = at if lands is None else names.setdefault(lands, len(names))
        return pltpu.make_async_remote_copy(
            src_ref=src, dst_ref=dst, send_sem=ssem.at[at], recv_sem=rsem.at[got],
            device_id=to, device_id_type=MESH,
        )

    sent = []

    def move(copy):
        copy.start()
        sent.append(copy)

    def go(*args):
        move(send(*args))

    barrier = pltpu.get_barrier_semaphore()
    for partner in (other, xn, yn, z1):
        pl.semaphore_signal(barrier, inc=1, device_id=partner, device_id_type=MESH)

    @pl.when(inner == 1)
    def _():
        pl.semaphore_signal(barrier, inc=1, device_id=z3, device_id_type=MESH)

    inputs = [
        pltpu.make_async_copy(src, dst, load_sem.at[6 + at])
        for at, (src, dst) in enumerate(((ids_hbm, ids_ref), (gw_hbm, gw_ref), (tok_hbm, tok_ref)))
    ]
    for load in inputs:
        load.start()
    h0, h1 = pl.ds(core * half, half), pl.ds((1 - core) * half, half)
    loads = []
    for at, (src, cols) in enumerate(((wg_ref, pl.ds(0, ff)), (wu_ref, pl.ds(ff, ff)))):
        for side, deep in enumerate((h0, h1)):
            loads.append(pltpu.make_async_copy(
                src.at[0, deep], wgu.at[pl.ds(side * half, half), cols], load_sem.at[2 * at + side]))
    for side, cols in enumerate((h0, h1)):
        cols = pl.ds(pl.multiple_of(cols.start, 128), half)
        loads.append(pltpu.make_async_copy(
            wd_ref.at[0, :, cols], wdn.at[:, pl.ds(side * half, half)], load_sem.at[4 + side]))
    for load in loads:
        load.start()

    inputs[0].wait()
    inputs[1].wait()
    expert_at = lax.broadcasted_iota(jnp.int32, (experts, tok), 0)
    chosen, weight = jnp.zeros((experts, tok), f32), jnp.zeros((experts, tok), f32)
    for k in range(ids_ref.shape[0]):
        hit = expert_at == ids_ref[k : k + 1, :]
        chosen += jnp.where(hit, 1.0, 0.0)
        weight += jnp.where(hit, gw_ref[k : k + 1, :], 0.0)
    before = lax.broadcasted_iota(jnp.int32, (tok, tok), 0) < lax.broadcasted_iota(jnp.int32, (tok, tok), 1)
    rank = jnp.dot(chosen.astype(bf), jnp.where(before, 1.0, 0.0).astype(bf), preferred_element_type=f32)
    tab[0, 0, 0:experts] = jnp.where(chosen > 0.0, rank, -1.0).astype(bf)
    tab[0, 0, experts : 2 * experts] = weight.astype(bf)

    inputs[2].wait()
    pl.semaphore_wait(barrier, 4 + inner)

    def block(d):
        return tok_ref if d == 0 else xo.at[d - 1]

    def piece(d, p):
        return tab.at[d, 0] if p == 2 else block(d).at[pl.ds(p * rows, rows)]

    def hop(name, lands, p, came, to):
        return send((name, p), piece(came, p), piece(lands, p), to, ("z", lands, p))

    def plane(d, p):
        if p == 2:
            go(("xt", d), tab.at[d, 0], tab.at[d, 1], xn)
            go(("yt", d), tab.at[d, 0], tab.at[d, 2], yn)
        else:
            here = pl.ds(p * rows, rows)
            go(("xf", d, p), block(d).at[here, left], xa.at[d, here], xn)
            go(("yf", d, p), block(d).at[here, right], yb.at[d, here], yn)

    order = (2, 0, 1)

    def begin(role):
        for p in order:
            move(hop("z own", 1 if role else 2, p, 0, z1))
            if role:
                move(hop("z far", 1, p, 0, z3))
            plane(0, p)

    slot_at = lax.broadcasted_iota(jnp.int32, (cap, tok), 0).astype(f32)

    def row(d, line, e, base):
        table = tab[d, line, base : base + experts].astype(f32)
        return jnp.sum(jnp.where(expert_at == e, table, 0.0), axis=0, keepdims=True)

    def pick(d, line, es):
        parts = [jnp.where(slot_at == row(d, line, e, 0), 1.0, 0.0).astype(bf) for e in es]
        return jnp.concatenate(parts, axis=0)

    def spread(d, line, e, values):
        w = jnp.where(slot_at == row(d, line, e, 0), row(d, line, e, experts), 0.0)
        return lax.dot_general(w.astype(bf), values, (((0,), (0,)), ((), ())), preferred_element_type=f32)

    def expect(name, ref):
        send(name, ref, ref, other).wait_recv()

    def arrive(role, d, p):
        expect(("z", d, p), piece(d, p))
        if role:
            lands, to = ((2, z1), (3, z3), (3, z1))[d - 1]
            move(hop("z on" + str(d), lands, p, d, to))
        plane(d, p)

    c1, c2, c3, c4 = (pl.ds(i * cap, cap) for i in range(4))
    lo, hi = pl.ds(0, half), pl.ds(half, half)

    def first(d):
        got = jnp.dot(pick(d, 0, (ep, ey)), block(d)[:, left], preferred_element_type=f32).astype(bf)
        rows_in[d, c1, left] = got[:cap]
        cy[d] = got[cap:]
        go(("yc", d), cy.at[d], rows_in.at[d, c3, left], yn)
        got = jnp.dot(pick(d, 0, (ep, ex)), block(d)[:, right], preferred_element_type=f32).astype(bf)
        rows_in[d, c1, right] = got[:cap]
        cx[d] = got[cap:]
        go(("xc", d), cx.at[d], rows_in.at[d, c2, right], xn)
        go(("g1", d), rows_in.at[d, c1, lo], rows_in.at[d, c1, hi], other)

    def cross_x(d):
        expect(("xt", d), tab.at[d, 1])
        for p in range(2):
            expect(("xf", d, p), xa.at[d, pl.ds(p * rows, rows)])
        got = jnp.dot(pick(d, 1, (ep, ey)), xa[d], preferred_element_type=f32).astype(bf)
        rows_in[d, c2, left] = got[:cap]
        ry[d] = got[cap:]
        go(("yr", d), ry.at[d], rows_in.at[d, c4, left], yn)

    def cross_y(d):
        expect(("yt", d), tab.at[d, 2])
        for p in range(2):
            expect(("yf", d, p), yb.at[d, pl.ds(p * rows, rows)])
        got = jnp.dot(pick(d, 2, (ep, ex)), yb[d], preferred_element_type=f32).astype(bf)
        rows_in[d, c3, right] = got[:cap]
        rx[d] = got[cap:]
        go(("xr", d), rx.at[d], rows_in.at[d, c4, right], xn)

    mid = pl.ds(cap, 2 * cap)

    def share_mid(d):
        expect(("xc", d), rows_in.at[d, c2, right])
        expect(("yc", d), rows_in.at[d, c3, left])
        go(("g2", d), rows_in.at[d, mid, lo], rows_in.at[d, mid, hi], other)

    def share_far(d):
        expect(("yr", d), rows_in.at[d, c4, left])
        expect(("xr", d), rows_in.at[d, c4, right])
        go(("g3", d), rows_in.at[d, c4, lo], rows_in.at[d, c4, hi], other)

    def compute(d):
        expect(("g1", d), rows_in.at[d, c1, hi])
        expect(("g2", d), rows_in.at[d, mid, hi])
        expect(("g3", d), rows_in.at[d, c4, hi])
        gu = jnp.dot(rows_in[d], wgu[...], preferred_element_type=f32)
        gate, up = gu[:, :ff], gu[:, ff:]
        hidden = (gate / (1.0 + jnp.exp(-gate)) * up).astype(bf)
        po[d] = jnp.dot(hidden, wdn[:, half:], preferred_element_type=f32).astype(bf)
        go(("p", d), po.at[d], pin.at[d], other)
        mine[d] = jnp.dot(hidden, wdn[:, :half], preferred_element_type=f32).astype(bf)

    def close(d):
        expect(("p", d), pin.at[d])
        res[d] = (mine[d].astype(f32) + pin[d].astype(f32)).astype(bf)
        go(("da", d), res.at[d, c4, left], rda.at[d], yn)
        go(("db", d), res.at[d, c4, right], rdb.at[d], xn)

    def direct(d):
        go(("cy", d), res.at[d, c3, left], rcy.at[d], yn)
        go(("cx", d), res.at[d, c2, right], rcx.at[d], xn)

    def relay_x(d):
        expect(("da", d), rda.at[d])
        fx[d] = (spread(d, 1, ep, res[d, c2, left]) + spread(d, 1, ey, rda[d])).astype(bf)
        go(("fx", d), fx.at[d], rfx.at[d], xn)

    def relay_y(d):
        expect(("db", d), rdb.at[d])
        fy[d] = (spread(d, 2, ep, res[d, c3, right]) + spread(d, 2, ex, rdb[d])).astype(bf)
        go(("fy", d), fy.at[d], rfy.at[d], yn)

    apart = (z + 1 - 2 * (z % 2), (z + 2) % nz, nz - 1 - z)
    def home(role, p, d):
        cols = right if p else left
        e, part_in, full = (ex, rcx, rfy) if p else (ey, rcy, rfx)
        expect(("cx" if p else "cy", d), part_in.at[d])
        expect(("fy" if p else "fx", d), full.at[d])
        total = spread(d, 0, ep, res[d, c1, cols]) + spread(d, 0, e, part_in[d]) + full[d].astype(f32)
        if d == 0:
            own[:, cols] = total
            return
        zs[d - 1, :, cols] = total.astype(bf)
        step = (d + 1) % 3 if role else d - 1
        go(("o", d, p), zs.at[d - 1, :, cols], zin.at[step, :, cols],
           {"ep": apart[step] * 4 + y * 2 + x}, ("s", step, p))

    def ready():
        for load in loads:
            load.wait()

    def finish():
        for p, cols in enumerate((left, right)):
            total = own[:, cols]
            for d in range(nz - 1):
                expect(("s", d, p), zin.at[d, :, cols])
                total += zin[d, :, cols].astype(f32)
            out_ref[:, cols] = total.astype(bf)
        for copy in sent:
            copy.wait_send()
        sent.clear()

    steps = {
        "F": first, "X": cross_x, "Y": cross_y, "T": share_mid, "U": share_far, "C": compute, "W": ready,
        "K": close, "L": direct, "R": relay_x, "Q": relay_y,
    }
    def step(role, word):
        at = [int(v) for v in word[1:]]
        if word[0] == "A":
            arrive(role, *at)
        elif word[0] in "HJ":
            home(role, "HJ".index(word[0]), *at)
        else:
            steps[word[0]](*at)

    for role, plan in enumerate(PLANS):
        @pl.when(inner == role)
        def _():
            begin(role)
            for word in plan:
                step(role, word)
            finish()


def multicast(tokens, gate_weights, expert_ids, w_gate, w_up, w_down):
    tok, half = tokens.shape
    experts = w_gate.shape[0] * lax.axis_size("ep")
    nz = lax.axis_size("ep") // 4
    part, width, ff = half // 2, w_gate.shape[1], w_gate.shape[2]
    cap = slot_count(tok, expert_ids.shape[1], experts)
    bf = jnp.bfloat16
    vmem, hbm = pl.BlockSpec(memory_space=pltpu.VMEM), pl.BlockSpec(memory_space=pl.ANY)
    compact, full = pltpu.VMEM((nz, cap, part), bf), pltpu.VMEM((nz, tok, part), bf)
    wide = pltpu.VMEM((nz, 4 * cap, half), bf)
    return pl.pallas_call(
        functools.partial(kernel, cap),
        out_shape=jax.ShapeDtypeStruct((tok, half), bf),
        in_specs=[hbm] * 6,
        out_specs=vmem,
        scratch_shapes=[
            pltpu.VMEM((tok, half), bf),
            pltpu.VMEM((expert_ids.shape[1], tok), jnp.float32),
            pltpu.VMEM((expert_ids.shape[1], tok), jnp.int32),
            pltpu.VMEM((nz - 1, tok, half), bf), full, full,
            pltpu.VMEM((nz, 4 * cap, width), bf),
            compact, compact, compact, compact,
            pltpu.VMEM((nz, 3, 2 * experts, tok), bf),
            pltpu.VMEM((width, 2 * ff), bf),
            pltpu.VMEM((ff, width), bf),
            wide, wide, wide, wide,
            compact, compact, compact, compact,
            full, full, full, full,
            pltpu.VMEM((nz - 1, tok, half), bf),
            pltpu.VMEM((nz - 1, tok, half), bf),
            pltpu.VMEM((tok, half), jnp.float32),
        ],
        compiler_params=pltpu.CompilerParams(
            collective_id=0, has_side_effects=True, vmem_limit_bytes=60 * 1024 * 1024
        ),
    )(tokens, gate_weights.T, expert_ids.T, w_gate, w_up, w_down)


def local(tokens, gate_weights, expert_ids, w_gate, w_up, w_down):
    tok_dev, half = tokens.shape
    devices, cores = lax.axis_size("ep"), lax.axis_size("half")
    experts = w_gate.shape[0] * devices
    cap = slot_count(tok_dev, expert_ids.shape[1], experts)
    fits = tok_dev * devices * half * 2 <= 8 * 1024 * 1024 and w_gate.shape[0] == 1
    shaped = cores == 2 and devices == 4 * 4 and tok_dev == 128
    tiled = cap % 16 == 0 and half % 256 == 0 and experts % 16 == 0 and w_gate.shape[2] % 128 == 0
    plan = multicast if fits and shaped and tiled else slots
    return plan(tokens, gate_weights, expert_ids, w_gate, w_up, w_down)


def solution(mesh):
    placed = (
        P("ep", "half"),
        P("ep", None),
        P("ep", None),
        P("ep", None, "half"),
        P("ep", None, "half"),
        P("ep", "half", None),
    )
    return jax.shard_map(
        local, mesh=mesh, in_specs=placed, out_specs=P("ep", "half"), check_vma=False
    )
```

```python
import functools

import jax
import jax.numpy as jnp
from jax import lax
from jax.experimental import pallas as pl
from jax.experimental.pallas import tpu as pltpu
from jax.sharding import PartitionSpec as P

MESH = pl.DeviceIdType.MESH


def slot_count(tok_dev, top, experts):
    return min(tok_dev, max(2, 5 * tok_dev * top // (4 * experts)))


def slots(tokens, gate_weights, expert_ids, w_gate, w_up, w_down):
    tok_dev, half_width = tokens.shape
    top = expert_ids.shape[1]
    local_experts = w_gate.shape[0]
    experts = local_experts * lax.axis_size("ep")
    capacity = slot_count(tok_dev, top, experts)
    flat_ids = expert_ids.reshape(-1)
    columns = jnp.arange(experts, dtype=jnp.int32)
    onehot = (flat_ids[:, None] == columns[None, :]).astype(jnp.int32)
    ranks = jnp.sum((jnp.cumsum(onehot, axis=0) - onehot) * onehot, axis=1)
    slot = flat_ids * capacity + ranks
    token_of_pair = jnp.arange(tok_dev * top, dtype=jnp.int32) // top
    token_table = jnp.zeros((experts * capacity,), jnp.int32).at[slot].set(token_of_pair)
    filled = (
        jnp.zeros((experts * capacity,), jnp.bfloat16)
        .at[slot]
        .set(jnp.ones((tok_dev * top,), jnp.bfloat16))
    )
    outgoing = (tokens[token_table] * filled[:, None]).reshape(experts, capacity, half_width)
    received = lax.all_to_all(outgoing, "ep", split_axis=0, concat_axis=0, tiled=True)
    count = received.shape[1]
    whole = lax.all_gather(received, "half", axis=2, tiled=True)
    width = whole.shape[2]
    grouped = whole.reshape(-1, local_experts, count, width)
    gate = jnp.einsum("secd,edf->secf", grouped, w_gate, preferred_element_type=jnp.float32)
    up = jnp.einsum("secd,edf->secf", grouped, w_up, preferred_element_type=jnp.float32)
    hidden = (jax.nn.silu(gate) * up).astype(jnp.bfloat16)
    partial_out = jnp.einsum("secf,efd->secd", hidden, w_down, preferred_element_type=jnp.float32)
    partial_out = partial_out.astype(jnp.bfloat16).reshape(experts, count, width)
    widened = lax.optimization_barrier(partial_out).astype(jnp.float32)
    summed = lax.psum_scatter(widened.astype(jnp.bfloat16), "half", scatter_dimension=2, tiled=True)
    answer = lax.all_to_all(summed, "ep", split_axis=0, concat_axis=0, tiled=True)
    picked = answer.reshape(experts * capacity, -1)[slot].reshape(tok_dev, top, -1)
    slot_out = picked.astype(jnp.float32)
    mixed = jnp.einsum("tk,tkx->tx", gate_weights, slot_out)
    return mixed.astype(jnp.bfloat16)


PLANS = (
    (
        "A12", "F0", "G0", "Y0", "X0", "A10", "A11", "U0", "F1", "G1", "A22", "A20", "T0", "A21",
        "F2", "G2", "A32", "A30", "X2", "Y2", "W", "C0", "A31", "F3", "G3", "U2", "T2", "Y3", "X3",
        "X1", "C2", "T3", "D2", "Y1", "U3", "K2", "L2", "T1", "C3", "D3", "Q2", "K3", "R2", "U1",
        "C1", "D1", "Q3", "L3", "J2", "K1", "R3", "H2", "D0", "J3", "Q1", "K0", "L1", "H3", "R1",
        "J1", "Q0", "L0", "R0", "H1", "J0", "H0",
    ),
    (
        "A22", "F0", "A12", "A10", "A20", "A21", "A11", "A32", "A30", "F2", "G2", "A31", "X2", "Y2",
        "F3", "G3", "T2", "X3", "X1", "X0", "Y3", "U2", "F1", "Y1", "G1", "G0", "T3", "W", "C2",
        "U3", "Y0", "D2", "C3", "D3", "K2", "U1", "K3", "L3", "T1", "C1", "R3", "Q3", "U0", "R2",
        "D1", "K1", "T0", "H3", "L2", "J3", "L1", "N1", "C0", "R1", "Q2", "Q1", "N0", "H2", "D0",
        "K0", "L0", "J2", "J1", "M1", "Q0", "H1", "M0", "R0", "H0", "J0",
    ),
)
MERGE = ((1, 1), (0, 0))


def kernel(cap, *refs):
    dma = pltpu.SemaphoreType.DMA
    pl.run_scoped(functools.partial(body, cap, *refs), dma((12,)), dma((136,)), dma((136,)))


def body(cap, tok_hbm, gw_hbm, ids_hbm, wg_ref, wu_ref, wd_ref, out_ref,
         tok_ref, gw_ref, ids_ref, xo, xa, yb, rows_in, cx, cy, rx, ry, tab, near, seen, wgu, wdn, hid, po, pin, mine, res,
         rda, rdb, rcx, rcy, fx, fy, rfx, rfy, zs, zin, zm, own, load_sem, ssem, rsem):
    ep = lax.axis_index("ep")
    core = lax.axis_index("half")
    x, y, z = ep % 2, (ep // 2) % 2, ep // 4
    tok, half = out_ref.shape
    part, rows, ff = half // 2, tok // 2, wg_ref.shape[2]
    experts = tab.shape[1] // 2
    nz = tab.shape[0]
    f32, bf = jnp.float32, jnp.bfloat16
    inner = ((z + 1) // 2) % 2
    ex, ey, ed = z * 4 + y * 2 + (1 - x), z * 4 + (1 - y) * 2 + x, z * 4 + (1 - y) * 2 + (1 - x)
    other, xn, yn = {"half": 1 - core}, {"ep": ex}, {"ep": ey}
    z1 = {"ep": (z + 1 - 2 * (z % 2)) * 4 + y * 2 + x}
    z3 = {"ep": (nz - 1 - z) * 4 + y * 2 + x}
    left, right = pl.ds(0, part), pl.ds(part, part)
    names = {}

    def send(name, src, dst, to, lands=None):
        at = names.setdefault(name, len(names))
        got = at if lands is None else names.setdefault(lands, len(names))
        return pltpu.make_async_remote_copy(
            src_ref=src, dst_ref=dst, send_sem=ssem.at[at], recv_sem=rsem.at[got],
            device_id=to, device_id_type=MESH,
        )

    sent = []

    def move(copy):
        copy.start()
        sent.append(copy)

    def go(*args):
        move(send(*args))

    barrier = pltpu.get_barrier_semaphore()
    for partner in (other, xn, yn, z1):
        pl.semaphore_signal(barrier, inc=1, device_id=partner, device_id_type=MESH)

    @pl.when(inner == 1)
    def _():
        pl.semaphore_signal(barrier, inc=1, device_id=z3, device_id_type=MESH)

    inputs = [
        pltpu.make_async_copy(src, dst, load_sem.at[6 + at])
        for at, (src, dst) in enumerate(((ids_hbm, ids_ref), (gw_hbm, gw_ref), (tok_hbm, tok_ref)))
    ]
    for load in inputs:
        load.start()
    h0, h1 = pl.ds(core * half, half), pl.ds((1 - core) * half, half)
    loads = []
    for at, (src, cols) in enumerate(((wg_ref, pl.ds(0, ff)), (wu_ref, pl.ds(ff, ff)))):
        for side, deep in enumerate((h0, h1)):
            loads.append(pltpu.make_async_copy(
                src.at[0, deep], wgu.at[pl.ds(side * half, half), cols], load_sem.at[2 * at + side]))
    for side, cols in enumerate((h0, h1)):
        cols = pl.ds(pl.multiple_of(cols.start, 128), half)
        loads.append(pltpu.make_async_copy(
            wd_ref.at[0, :, cols], wdn.at[:, pl.ds(side * half, half)], load_sem.at[4 + side]))
    for load in loads:
        load.start()

    inputs[0].wait()
    inputs[1].wait()
    expert_at = lax.broadcasted_iota(jnp.int32, (experts, tok), 0)
    chosen, weight = jnp.zeros((experts, tok), f32), jnp.zeros((experts, tok), f32)
    for k in range(ids_ref.shape[0]):
        hit = expert_at == ids_ref[k : k + 1, :]
        chosen += jnp.where(hit, 1.0, 0.0)
        weight += jnp.where(hit, gw_ref[k : k + 1, :], 0.0)
    before = lax.broadcasted_iota(jnp.int32, (tok, tok), 0) < lax.broadcasted_iota(jnp.int32, (tok, tok), 1)
    rank = jnp.dot(chosen.astype(bf), jnp.where(before, 1.0, 0.0).astype(bf), preferred_element_type=f32)
    tab[0, 0:experts] = jnp.where(chosen > 0.0, rank, -1.0).astype(bf)
    tab[0, experts : 2 * experts] = weight.astype(bf)

    inputs[2].wait()
    pl.semaphore_wait(barrier, 4 + inner)

    slot_at = lax.broadcasted_iota(jnp.int32, (cap, tok), 0).astype(f32)
    tile_at = lax.broadcasted_iota(jnp.int32, (16, tok), 0)

    def lookup(table, e, base):
        half_of = table[base * experts : (base + 1) * experts].astype(f32)
        return jnp.sum(jnp.where(expert_at == e, half_of, 0.0), axis=0, keepdims=True)

    def row(d, line, who, base):
        if line == 0:
            return lookup(tab[d], {"me": ep, "x": ex, "y": ey}[who], base)
        at = 2 * base + (who != "me")
        return seen[d, line - 1].astype(f32)[at : at + 1]

    def pick(d, line, es):
        parts = [jnp.where(slot_at == row(d, line, e, 0), 1.0, 0.0).astype(bf) for e in es]
        return jnp.concatenate(parts, axis=0)

    def spread(d, line, e, values):
        w = jnp.where(slot_at == row(d, line, e, 0), row(d, line, e, 1), 0.0)
        return lax.dot_general(w.astype(bf), values, (((0,), (0,)), ((), ())), preferred_element_type=f32)

    def block(d):
        return tok_ref if d == 0 else xo.at[d - 1]

    def piece(d, p):
        return tab.at[d] if p == 2 else block(d).at[pl.ds(p * rows, rows)]

    def hop(name, lands, p, came, to):
        return send((name, p), piece(came, p), piece(lands, p), to, ("z", lands, p))

    def plane(d, p):
        if p == 2:
            for line, to, mark in ((1, xn, "xt"), (2, yn, "yt")):
                tile = jnp.zeros((16, tok), f32)
                for at, e in enumerate((ex if line == 1 else ey, ed)):
                    for base in range(2):
                        tile = jnp.where(tile_at == at + 2 * base, lookup(tab[d], e, base), tile)
                near[d, line - 1] = tile.astype(bf)
                go((mark, d), near.at[d, line - 1], seen.at[d, line - 1], to)
        else:
            here = pl.ds(p * rows, rows)
            go(("xf", d, p), block(d).at[here, left], xa.at[d, here], xn)
            go(("yf", d, p), block(d).at[here, right], yb.at[d, here], yn)

    order = (2, 0, 1)

    def begin(role):
        for p in order:
            move(hop("z own", 1 if role else 2, p, 0, z1))
            if role:
                move(hop("z far", 1, p, 0, z3))
            plane(0, p)

    def expect(name, ref):
        send(name, ref, ref, other).wait_recv()

    def arrive(role, d, p):
        expect(("z", d, p), piece(d, p))
        if role:
            lands, to = ((2, z1), (3, z3), (3, z1))[d - 1]
            move(hop("z on" + str(d), lands, p, d, to))
        plane(d, p)

    c1, c2, c3, c4 = (pl.ds(i * cap, cap) for i in range(4))
    lo, hi = pl.ds(0, half), pl.ds(half, half)

    def first_y(d):
        got = jnp.dot(pick(d, 0, ("me", "y")), block(d)[:, left], preferred_element_type=f32).astype(bf)
        rows_in[d, c1, left] = got[:cap]
        cy[d] = got[cap:]
        go(("yc", d), cy.at[d], rows_in.at[d, c3, left], yn)

    def first_x(d):
        got = jnp.dot(pick(d, 0, ("me", "x")), block(d)[:, right], preferred_element_type=f32).astype(bf)
        rows_in[d, c1, right] = got[:cap]
        cx[d] = got[cap:]
        go(("xc", d), cx.at[d], rows_in.at[d, c2, right], xn)
        go(("g1", d), rows_in.at[d, c1, lo], rows_in.at[d, c1, hi], other)

    def cross_x(d):
        expect(("xt", d), seen.at[d, 0])
        for p in range(2):
            expect(("xf", d, p), xa.at[d, pl.ds(p * rows, rows)])
        got = jnp.dot(pick(d, 1, ("me", "y")), xa[d], preferred_element_type=f32).astype(bf)
        rows_in[d, c2, left] = got[:cap]
        ry[d] = got[cap:]
        go(("yr", d), ry.at[d], rows_in.at[d, c4, left], yn)

    def cross_y(d):
        expect(("yt", d), seen.at[d, 1])
        for p in range(2):
            expect(("yf", d, p), yb.at[d, pl.ds(p * rows, rows)])
        got = jnp.dot(pick(d, 2, ("me", "x")), yb[d], preferred_element_type=f32).astype(bf)
        rows_in[d, c3, right] = got[:cap]
        rx[d] = got[cap:]
        go(("xr", d), rx.at[d], rows_in.at[d, c4, right], xn)

    mid = pl.ds(cap, 2 * cap)

    def share_mid(d):
        expect(("xc", d), rows_in.at[d, c2, right])
        expect(("yc", d), rows_in.at[d, c3, left])
        go(("g2", d), rows_in.at[d, mid, lo], rows_in.at[d, mid, hi], other)

    def share_far(d):
        expect(("yr", d), rows_in.at[d, c4, left])
        expect(("xr", d), rows_in.at[d, c4, right])
        go(("g3", d), rows_in.at[d, c4, lo], rows_in.at[d, c4, hi], other)

    def compute(d):
        expect(("g1", d), rows_in.at[d, c1, hi])
        expect(("g2", d), rows_in.at[d, mid, hi])
        expect(("g3", d), rows_in.at[d, c4, hi])
        gu = jnp.dot(rows_in[d], wgu[...], preferred_element_type=f32)
        gate, up = gu[:, :ff], gu[:, ff:]
        hid[d] = (gate / (1.0 + jnp.exp(-gate)) * up).astype(bf)

    def project(d):
        po[d] = jnp.dot(hid[d], wdn[:, half:], preferred_element_type=f32).astype(bf)
        go(("p", d), po.at[d], pin.at[d], other)
        mine[d] = jnp.dot(hid[d], wdn[:, :half], preferred_element_type=f32).astype(bf)

    def close(d):
        expect(("p", d), pin.at[d])
        res[d] = (mine[d].astype(f32) + pin[d].astype(f32)).astype(bf)
        go(("da", d), res.at[d, c4, left], rda.at[d], yn)
        go(("db", d), res.at[d, c4, right], rdb.at[d], xn)

    def direct(d):
        go(("cy", d), res.at[d, c3, left], rcy.at[d], yn)
        go(("cx", d), res.at[d, c2, right], rcx.at[d], xn)

    def relay_x(d):
        expect(("da", d), rda.at[d])
        fx[d] = (spread(d, 1, "me", res[d, c2, left]) + spread(d, 1, "y", rda[d])).astype(bf)
        go(("fx", d), fx.at[d], rfx.at[d], xn)

    def relay_y(d):
        expect(("db", d), rdb.at[d])
        fy[d] = (spread(d, 2, "me", res[d, c3, right]) + spread(d, 2, "x", rdb[d])).astype(bf)
        go(("fy", d), fy.at[d], rfy.at[d], yn)

    apart = (z + 1 - 2 * (z % 2), (z + 2) % nz, nz - 1 - z)
    def home(role, p, d):
        cols = right if p else left
        e, part_in, full = ("x", rcx, rfy) if p else ("y", rcy, rfx)
        expect(("cx" if p else "cy", d), part_in.at[d])
        expect(("fy" if p else "fx", d), full.at[d])
        total = spread(d, 0, "me", res[d, c1, cols]) + spread(d, 0, e, part_in[d]) + full[d].astype(f32)
        if d == 0:
            own[:, cols] = total
            return
        zs[d - 1, :, cols] = total.astype(bf)
        if role == 0 and d > 1 and MERGE[d - 2][p]:
            go(("o", d, p), zs.at[d - 1, :, cols], zm.at[d - 2, :, cols], z1, ("m", d, p))
        elif role == 0 or not ((d == 1 and MERGE[0][p]) or (d == 3 and MERGE[1][p])):
            forward(role, p, d)

    def forward(role, p, d):
        cols = right if p else left
        step = (d + 1) % 3 if role else d - 1
        go(("o", d, p), zs.at[d - 1, :, cols], zin.at[step, :, cols],
           {"ep": apart[step] * 4 + y * 2 + x}, ("s", step, p))

    def merge(d, p):
        at, cols = (0 if d == 1 else 1), right if p else left
        if MERGE[at][p]:
            expect(("m", at + 2, p), zm.at[at, :, cols])
            zs[d - 1, :, cols] = (zs[d - 1, :, cols].astype(f32) + zm[at, :, cols].astype(f32)).astype(bf)
            forward(1, p, d)

    def ready():
        for load in loads:
            load.wait()

    def finish(role):
        for p, cols in enumerate((left, right)):
            total = own[:, cols]
            for step in range(nz - 1):
                if (role == 0 and step == 2 and MERGE[1][p]) or (role == 1 and step == 1 and MERGE[0][p]):
                    continue
                expect(("s", step, p), zin.at[step, :, cols])
                total += zin[step, :, cols].astype(f32)
            out_ref[:, cols] = total.astype(bf)
        for copy in sent:
            copy.wait_send()
        sent.clear()

    steps = {
        "F": first_y, "G": first_x, "X": cross_x, "Y": cross_y, "T": share_mid, "U": share_far, "W": ready,
        "C": compute, "D": project, "K": close, "L": direct, "R": relay_x, "Q": relay_y,
        "M": functools.partial(merge, 1), "N": functools.partial(merge, 3),
    }

    def step(role, word):
        at = [int(v) for v in word[1:]]
        if word[0] == "A":
            arrive(role, *at)
        elif word[0] in "HJ":
            home(role, "HJ".index(word[0]), *at)
        else:
            steps[word[0]](*at)

    for role, plan in enumerate(PLANS):
        @pl.when(inner == role)
        def _():
            begin(role)
            for word in plan:
                step(role, word)
            finish(role)


def multicast(tokens, gate_weights, expert_ids, w_gate, w_up, w_down):
    tok, half = tokens.shape
    experts = w_gate.shape[0] * lax.axis_size("ep")
    nz = lax.axis_size("ep") // 4
    part, width, ff = half // 2, w_gate.shape[1], w_gate.shape[2]
    cap = slot_count(tok, expert_ids.shape[1], experts)
    bf = jnp.bfloat16
    vmem, hbm = pl.BlockSpec(memory_space=pltpu.VMEM), pl.BlockSpec(memory_space=pl.ANY)
    compact, full = pltpu.VMEM((nz, cap, part), bf), pltpu.VMEM((nz, tok, part), bf)
    wide = pltpu.VMEM((nz, 4 * cap, half), bf)
    return pl.pallas_call(
        functools.partial(kernel, cap),
        out_shape=pltpu.VMEM((tok, half), bf),
        in_specs=[hbm] * 6,
        out_specs=vmem,
        scratch_shapes=[
            pltpu.VMEM((tok, half), bf),
            pltpu.VMEM((expert_ids.shape[1], tok), jnp.float32),
            pltpu.VMEM((expert_ids.shape[1], tok), jnp.int32),
            pltpu.VMEM((nz - 1, tok, half), bf), full, full,
            pltpu.VMEM((nz, 4 * cap, width), bf),
            compact, compact, compact, compact,
            pltpu.VMEM((nz, 2 * experts, tok), bf),
            pltpu.VMEM((nz, 2, 16, tok), bf),
            pltpu.VMEM((nz, 2, 16, tok), bf),
            pltpu.VMEM((width, 2 * ff), bf),
            pltpu.VMEM((ff, width), bf),
            pltpu.VMEM((nz, 4 * cap, ff), bf),
            wide, wide, wide, wide,
            compact, compact, compact, compact,
            full, full, full, full,
            pltpu.VMEM((nz - 1, tok, half), bf),
            pltpu.VMEM((nz - 1, tok, half), bf),
            pltpu.VMEM((2, tok, half), bf),
            pltpu.VMEM((tok, half), jnp.float32),
        ],
        compiler_params=pltpu.CompilerParams(
            collective_id=0, has_side_effects=True, vmem_limit_bytes=60 * 1024 * 1024
        ),
    )(tokens, gate_weights.T, expert_ids.T, w_gate, w_up, w_down)


def local(tokens, gate_weights, expert_ids, w_gate, w_up, w_down):
    tok_dev, half = tokens.shape
    devices, cores = lax.axis_size("ep"), lax.axis_size("half")
    experts = w_gate.shape[0] * devices
    cap = slot_count(tok_dev, expert_ids.shape[1], experts)
    fits = tok_dev * devices * half * 2 <= 8 * 1024 * 1024 and w_gate.shape[0] == 1
    shaped = cores == 2 and devices == 4 * 4 and tok_dev == 128
    tiled = cap % 16 == 0 and half % 256 == 0 and experts % 16 == 0 and w_gate.shape[2] % 128 == 0
    plan = multicast if fits and shaped and tiled else slots
    return plan(tokens, gate_weights, expert_ids, w_gate, w_up, w_down)


def solution(mesh):
    placed = (
        P("ep", "half"),
        P("ep", None),
        P("ep", None),
        P("ep", None, "half"),
        P("ep", None, "half"),
        P("ep", "half", None),
    )
    return jax.shard_map(
        local, mesh=mesh, in_specs=placed, out_specs=P("ep", "half"), check_vma=False
    )
```

```python
import functools

import jax
import jax.numpy as jnp
from jax import lax
from jax.experimental import pallas as pl
from jax.experimental.pallas import tpu as pltpu
from jax.sharding import PartitionSpec as P

MESH = pl.DeviceIdType.MESH


def slot_count(tok_dev, top, experts):
    return min(tok_dev, max(2, 5 * tok_dev * top // (4 * experts)))


def slots(tokens, gate_weights, expert_ids, w_gate, w_up, w_down):
    tok_dev, half_width = tokens.shape
    top = expert_ids.shape[1]
    local_experts = w_gate.shape[0]
    experts = local_experts * lax.axis_size("ep")
    capacity = slot_count(tok_dev, top, experts)
    flat_ids = expert_ids.reshape(-1)
    columns = jnp.arange(experts, dtype=jnp.int32)
    onehot = (flat_ids[:, None] == columns[None, :]).astype(jnp.int32)
    ranks = jnp.sum((jnp.cumsum(onehot, axis=0) - onehot) * onehot, axis=1)
    slot = flat_ids * capacity + ranks
    token_of_pair = jnp.arange(tok_dev * top, dtype=jnp.int32) // top
    token_table = jnp.zeros((experts * capacity,), jnp.int32).at[slot].set(token_of_pair)
    filled = (
        jnp.zeros((experts * capacity,), jnp.bfloat16)
        .at[slot]
        .set(jnp.ones((tok_dev * top,), jnp.bfloat16))
    )
    outgoing = (tokens[token_table] * filled[:, None]).reshape(experts, capacity, half_width)
    received = lax.all_to_all(outgoing, "ep", split_axis=0, concat_axis=0, tiled=True)
    count = received.shape[1]
    whole = lax.all_gather(received, "half", axis=2, tiled=True)
    width = whole.shape[2]
    grouped = whole.reshape(-1, local_experts, count, width)
    gate = jnp.einsum("secd,edf->secf", grouped, w_gate, preferred_element_type=jnp.float32)
    up = jnp.einsum("secd,edf->secf", grouped, w_up, preferred_element_type=jnp.float32)
    hidden = (jax.nn.silu(gate) * up).astype(jnp.bfloat16)
    partial_out = jnp.einsum("secf,efd->secd", hidden, w_down, preferred_element_type=jnp.float32)
    partial_out = partial_out.astype(jnp.bfloat16).reshape(experts, count, width)
    widened = lax.optimization_barrier(partial_out).astype(jnp.float32)
    summed = lax.psum_scatter(widened.astype(jnp.bfloat16), "half", scatter_dimension=2, tiled=True)
    answer = lax.all_to_all(summed, "ep", split_axis=0, concat_axis=0, tiled=True)
    picked = answer.reshape(experts * capacity, -1)[slot].reshape(tok_dev, top, -1)
    slot_out = picked.astype(jnp.float32)
    mixed = jnp.einsum("tk,tkx->tx", gate_weights, slot_out)
    return mixed.astype(jnp.bfloat16)


PLANS = (
    (
        "A12", "F0", "G0", "A10", "Y0", "A22", "A11", "F1", "G1", "A20", "Y1", "X1", "A21", "F2",
        "A32", "G2", "A30", "T1", "Y2", "U1", "X2", "A31", "W", "C1", "F3", "G3", "D1", "T2", "U2",
        "Y3", "X3", "K1", "C2", "D2", "K2", "T3", "X0", "U3", "L2", "C3", "D3", "R2", "K3", "U0",
        "Q2", "T0", "H20", "L3", "C0", "R3", "H21", "L1", "J20", "R1", "Q3", "D0", "J21", "K0",
        "H30", "H31", "J30", "Q1", "J31", "L0", "H10", "J10", "R0", "Q0", "H11", "J11", "H00",
        "J00", "H01", "J01",
    ),
    (
        "A22", "F0", "G0", "A12", "A20", "A10", "A32", "A11", "A21", "F2", "A30", "G2", "Y2", "A31",
        "X2", "Y1", "F1", "T2", "X1", "G1", "X0", "F3", "Y0", "Y3", "G3", "U2", "W", "C2", "X3",
        "U1", "T1", "D2", "K2", "C1", "L2", "D1", "T0", "K1", "Q2", "R2", "U3", "L1", "T3", "U0",
        "C3", "R1", "D3", "H20", "K3", "H21", "Q1", "L3", "J20", "C0", "H10", "R3", "M00", "D0",
        "J21", "J10", "Q3", "K0", "H11", "M01", "M10", "H30", "N00", "L0", "H31", "N01", "J30",
        "N10", "J31", "J11", "Q0", "N11", "R0", "M11", "J00", "H00", "J01", "H01",
    ),
)
MERGE = ((1, 1), (1, 1))


def kernel(cap, *refs):
    dma = pltpu.SemaphoreType.DMA
    pl.run_scoped(functools.partial(body, cap, *refs), dma((12,)), dma((180,)), dma((180,)))


def body(cap, tok_hbm, gw_hbm, ids_hbm, wg_ref, wu_ref, wd_ref, out_ref,
         tok_ref, gw_ref, ids_ref, xo, xa, yb, rows_in, cx, cy, rx, ry, tab, near, seen, wgu, wdn, hid, po, pin, mine, res,
         rda, rdb, rcx, rcy, fx, fy, rfx, rfy, zs, zin, zm, acc, own, load_sem, ssem, rsem):
    ep = lax.axis_index("ep")
    core = lax.axis_index("half")
    x, y, z = ep % 2, (ep // 2) % 2, ep // 4
    tok, half = out_ref.shape
    part, rows, ff = half // 2, tok // 2, wg_ref.shape[2]
    experts = tab.shape[1] // 2
    nz = tab.shape[0]
    f32, bf = jnp.float32, jnp.bfloat16
    inner = ((z + 1) // 2) % 2
    ex, ey, ed = z * 4 + y * 2 + (1 - x), z * 4 + (1 - y) * 2 + x, z * 4 + (1 - y) * 2 + (1 - x)
    other, xn, yn = {"half": 1 - core}, {"ep": ex}, {"ep": ey}
    z1 = {"ep": (z + 1 - 2 * (z % 2)) * 4 + y * 2 + x}
    z3 = {"ep": (nz - 1 - z) * 4 + y * 2 + x}
    left, right = pl.ds(0, part), pl.ds(part, part)
    names = {}

    def send(name, src, dst, to, lands=None):
        at = names.setdefault(name, len(names))
        got = at if lands is None else names.setdefault(lands, len(names))
        return pltpu.make_async_remote_copy(
            src_ref=src, dst_ref=dst, send_sem=ssem.at[at], recv_sem=rsem.at[got],
            device_id=to, device_id_type=MESH,
        )

    sent = []

    def move(copy):
        copy.start()
        sent.append(copy)

    def go(*args):
        move(send(*args))

    barrier = pltpu.get_barrier_semaphore()
    for partner in (other, xn, yn, z1):
        pl.semaphore_signal(barrier, inc=1, device_id=partner, device_id_type=MESH)

    @pl.when(inner == 1)
    def _():
        pl.semaphore_signal(barrier, inc=1, device_id=z3, device_id_type=MESH)

    inputs = [
        pltpu.make_async_copy(src, dst, load_sem.at[6 + at])
        for at, (src, dst) in enumerate(((ids_hbm, ids_ref), (gw_hbm, gw_ref), (tok_hbm, tok_ref)))
    ]
    for load in inputs:
        load.start()
    h0, h1 = pl.ds(core * half, half), pl.ds((1 - core) * half, half)
    loads = []
    for at, (src, cols) in enumerate(((wg_ref, pl.ds(0, ff)), (wu_ref, pl.ds(ff, ff)))):
        for side, deep in enumerate((h0, h1)):
            loads.append(pltpu.make_async_copy(
                src.at[0, deep], wgu.at[pl.ds(side * half, half), cols], load_sem.at[2 * at + side]))
    for side, cols in enumerate((h0, h1)):
        cols = pl.ds(pl.multiple_of(cols.start, 128), half)
        loads.append(pltpu.make_async_copy(
            wd_ref.at[0, :, cols], wdn.at[:, pl.ds(side * half, half)], load_sem.at[4 + side]))
    for load in loads:
        load.start()

    inputs[0].wait()
    inputs[1].wait()
    expert_at = lax.broadcasted_iota(jnp.int32, (experts, tok), 0)
    chosen, weight = jnp.zeros((experts, tok), f32), jnp.zeros((experts, tok), f32)
    for k in range(ids_ref.shape[0]):
        hit = expert_at == ids_ref[k : k + 1, :]
        chosen += jnp.where(hit, 1.0, 0.0)
        weight += jnp.where(hit, gw_ref[k : k + 1, :], 0.0)
    before = lax.broadcasted_iota(jnp.int32, (tok, tok), 0) < lax.broadcasted_iota(jnp.int32, (tok, tok), 1)
    rank = jnp.dot(chosen.astype(bf), jnp.where(before, 1.0, 0.0).astype(bf), preferred_element_type=f32)
    tab[0, 0:experts] = jnp.where(chosen > 0.0, rank, -1.0).astype(bf)
    tab[0, experts : 2 * experts] = weight.astype(bf)

    inputs[2].wait()
    pl.semaphore_wait(barrier, 4 + inner)

    slot_at = lax.broadcasted_iota(jnp.int32, (cap, tok), 0).astype(f32)
    tile_at = lax.broadcasted_iota(jnp.int32, (16, tok), 0)

    def lookup(table, e, base):
        half_of = table[base * experts : (base + 1) * experts].astype(f32)
        return jnp.sum(jnp.where(expert_at == e, half_of, 0.0), axis=0, keepdims=True)

    def row(d, line, who, base):
        if line == 0:
            return lookup(tab[d], {"me": ep, "x": ex, "y": ey}[who], base)
        at = 2 * base + (who != "me")
        return seen[d, line - 1].astype(f32)[at : at + 1]

    def pick(d, line, es):
        parts = [jnp.where(slot_at == row(d, line, e, 0), 1.0, 0.0).astype(bf) for e in es]
        return jnp.concatenate(parts, axis=0)

    def spread(d, line, e, values):
        w = jnp.where(slot_at == row(d, line, e, 0), row(d, line, e, 1), 0.0)
        return lax.dot_general(w.astype(bf), values, (((0,), (0,)), ((), ())), preferred_element_type=f32)

    def block(d):
        return tok_ref if d == 0 else xo.at[d - 1]

    def piece(d, p):
        return tab.at[d] if p == 2 else block(d).at[pl.ds(p * rows, rows)]

    def hop(name, lands, p, came, to):
        return send((name, p), piece(came, p), piece(lands, p), to, ("z", lands, p))

    def plane(d, p):
        if p == 2:
            for line, to, mark in ((1, xn, "xt"), (2, yn, "yt")):
                tile = jnp.zeros((16, tok), f32)
                for at, e in enumerate((ex if line == 1 else ey, ed)):
                    for base in range(2):
                        tile = jnp.where(tile_at == at + 2 * base, lookup(tab[d], e, base), tile)
                near[d, line - 1] = tile.astype(bf)
                go((mark, d), near.at[d, line - 1], seen.at[d, line - 1], to)
        else:
            here = pl.ds(p * rows, rows)
            go(("xf", d, p), block(d).at[here, left], xa.at[d, here], xn)
            go(("yf", d, p), block(d).at[here, right], yb.at[d, here], yn)

    order = (2, 0, 1)

    def begin(role):
        for p in order:
            move(hop("z own", 1 if role else 2, p, 0, z1))
            if role:
                move(hop("z far", 1, p, 0, z3))
            plane(0, p)

    def expect(name, ref):
        send(name, ref, ref, other).wait_recv()

    def arrive(role, d, p):
        expect(("z", d, p), piece(d, p))
        if role:
            lands, to = ((2, z1), (3, z3), (3, z1))[d - 1]
            move(hop("z on" + str(d), lands, p, d, to))
        plane(d, p)

    c1, c2, c3, c4 = (pl.ds(i * cap, cap) for i in range(4))
    lo, hi = pl.ds(0, half), pl.ds(half, half)

    def first_y(d):
        got = jnp.dot(pick(d, 0, ("me", "y")), block(d)[:, left], preferred_element_type=f32).astype(bf)
        rows_in[d, c1, left] = got[:cap]
        cy[d] = got[cap:]
        go(("yc", d), cy.at[d], rows_in.at[d, c3, left], yn)

    def first_x(d):
        got = jnp.dot(pick(d, 0, ("me", "x")), block(d)[:, right], preferred_element_type=f32).astype(bf)
        rows_in[d, c1, right] = got[:cap]
        cx[d] = got[cap:]
        go(("xc", d), cx.at[d], rows_in.at[d, c2, right], xn)
        go(("g1", d), rows_in.at[d, c1, lo], rows_in.at[d, c1, hi], other)

    def cross_x(d):
        expect(("xt", d), seen.at[d, 0])
        for p in range(2):
            expect(("xf", d, p), xa.at[d, pl.ds(p * rows, rows)])
        got = jnp.dot(pick(d, 1, ("me", "y")), xa[d], preferred_element_type=f32).astype(bf)
        rows_in[d, c2, left] = got[:cap]
        ry[d] = got[cap:]
        go(("yr", d), ry.at[d], rows_in.at[d, c4, left], yn)

    def cross_y(d):
        expect(("yt", d), seen.at[d, 1])
        for p in range(2):
            expect(("yf", d, p), yb.at[d, pl.ds(p * rows, rows)])
        got = jnp.dot(pick(d, 2, ("me", "x")), yb[d], preferred_element_type=f32).astype(bf)
        rows_in[d, c3, right] = got[:cap]
        rx[d] = got[cap:]
        go(("xr", d), rx.at[d], rows_in.at[d, c4, right], xn)

    mid = pl.ds(cap, 2 * cap)

    def share_mid(d):
        expect(("xc", d), rows_in.at[d, c2, right])
        expect(("yc", d), rows_in.at[d, c3, left])
        go(("g2", d), rows_in.at[d, mid, lo], rows_in.at[d, mid, hi], other)

    def share_far(d):
        expect(("yr", d), rows_in.at[d, c4, left])
        expect(("xr", d), rows_in.at[d, c4, right])
        go(("g3", d), rows_in.at[d, c4, lo], rows_in.at[d, c4, hi], other)

    def compute(d):
        expect(("g1", d), rows_in.at[d, c1, hi])
        expect(("g2", d), rows_in.at[d, mid, hi])
        expect(("g3", d), rows_in.at[d, c4, hi])
        gu = jnp.dot(rows_in[d], wgu[...], preferred_element_type=f32)
        gate, up = gu[:, :ff], gu[:, ff:]
        hid[d] = (gate / (1.0 + jnp.exp(-gate)) * up).astype(bf)

    rest = pl.ds(0, 3 * cap)

    def project(d):
        po[d] = jnp.dot(hid[d], wdn[:, half:], preferred_element_type=f32).astype(bf)
        go(("pf", d), po.at[d, c4], pin.at[d, c4], other)
        go(("p", d), po.at[d, rest], pin.at[d, rest], other)
        mine[d] = jnp.dot(hid[d], wdn[:, :half], preferred_element_type=f32).astype(bf)

    def close(d):
        expect(("pf", d), pin.at[d, c4])
        res[d, c4] = (mine[d, c4].astype(f32) + pin[d, c4].astype(f32)).astype(bf)
        go(("da", d), res.at[d, c4, left], rda.at[d], yn)
        go(("db", d), res.at[d, c4, right], rdb.at[d], xn)

    def direct(d):
        expect(("p", d), pin.at[d, rest])
        res[d, rest] = (mine[d, rest].astype(f32) + pin[d, rest].astype(f32)).astype(bf)
        go(("cy", d), res.at[d, c3, left], rcy.at[d], yn)
        go(("cx", d), res.at[d, c2, right], rcx.at[d], xn)

    bands = {q: pl.ds(q * rows, rows) for q in range(2)}

    def relay_x(d):
        expect(("da", d), rda.at[d])
        fx[d] = (spread(d, 1, "me", res[d, c2, left]) + spread(d, 1, "y", rda[d])).astype(bf)
        for q in bands:
            go(("fx", d, q), fx.at[d, bands[q]], rfx.at[d, bands[q]], xn)

    def relay_y(d):
        expect(("db", d), rdb.at[d])
        fy[d] = (spread(d, 2, "me", res[d, c3, right]) + spread(d, 2, "x", rdb[d])).astype(bf)
        for q in bands:
            go(("fy", d, q), fy.at[d, bands[q]], rfy.at[d, bands[q]], yn)

    apart = (z + 1 - 2 * (z % 2), (z + 2) % nz, nz - 1 - z)
    def home(role, p, d, q):
        cols, band = right if p else left, bands[q]
        e, part_in, full = ("x", rcx, rfy) if p else ("y", rcy, rfx)
        if q == 0:
            expect(("cx" if p else "cy", d), part_in.at[d])
            acc[d, p] = spread(d, 0, "me", res[d, c1, cols]) + spread(d, 0, e, part_in[d])
        expect(("fy" if p else "fx", d, q), full.at[d, band])
        total = acc[d, p, band] + full[d, band].astype(f32)
        if d == 0:
            own[band, cols] = total
            return
        zs[d - 1, band, cols] = total.astype(bf)
        if role == 0 and d > 1 and MERGE[d - 2][p]:
            go(("o", d, p, q), zs.at[d - 1, band, cols], zm.at[d - 2, band, cols], z1, ("m", d, p, q))
        elif role == 0 or not ((d == 1 and MERGE[0][p]) or (d == 3 and MERGE[1][p])):
            forward(role, p, d, q)

    def forward(role, p, d, q):
        cols, band = right if p else left, bands[q]
        step = (d + 1) % 3 if role else d - 1
        go(("o", d, p, q), zs.at[d - 1, band, cols], zin.at[step, band, cols],
           {"ep": apart[step] * 4 + y * 2 + x}, ("s", step, p, q))

    def merge(d, p, q):
        at, cols, band = (0 if d == 1 else 1), right if p else left, bands[q]
        if MERGE[at][p]:
            expect(("m", at + 2, p, q), zm.at[at, band, cols])
            zs[d - 1, band, cols] = (zs[d - 1, band, cols].astype(f32) + zm[at, band, cols].astype(f32)).astype(bf)
            forward(1, p, d, q)

    def ready():
        for load in loads:
            load.wait()

    def finish(role):
        for p, cols in enumerate((left, right)):
            total = own[:, cols]
            for step in range(nz - 1):
                if (role == 0 and step == 2 and MERGE[1][p]) or (role == 1 and step == 1 and MERGE[0][p]):
                    continue
                for q in bands:
                    expect(("s", step, p, q), zin.at[step, bands[q], cols])
                total += zin[step, :, cols].astype(f32)
            out_ref[:, cols] = total.astype(bf)
        for copy in sent:
            copy.wait_send()
        sent.clear()

    steps = {
        "F": first_y, "G": first_x, "X": cross_x, "Y": cross_y, "T": share_mid, "U": share_far, "W": ready,
        "C": compute, "D": project, "K": close, "L": direct, "R": relay_x, "Q": relay_y,
        "M": functools.partial(merge, 1), "N": functools.partial(merge, 3),
    }

    def step(role, word):
        at = [int(v) for v in word[1:]]
        if word[0] == "A":
            arrive(role, *at)
        elif word[0] in "HJ":
            home(role, "HJ".index(word[0]), *at)
        else:
            steps[word[0]](*at)

    for role, plan in enumerate(PLANS):
        @pl.when(inner == role)
        def _():
            begin(role)
            for word in plan:
                step(role, word)
            finish(role)


def multicast(tokens, gate_weights, expert_ids, w_gate, w_up, w_down):
    tok, half = tokens.shape
    experts = w_gate.shape[0] * lax.axis_size("ep")
    nz = lax.axis_size("ep") // 4
    part, width, ff = half // 2, w_gate.shape[1], w_gate.shape[2]
    cap = slot_count(tok, expert_ids.shape[1], experts)
    bf = jnp.bfloat16
    vmem, hbm = pl.BlockSpec(memory_space=pltpu.VMEM), pl.BlockSpec(memory_space=pl.ANY)
    compact, full = pltpu.VMEM((nz, cap, part), bf), pltpu.VMEM((nz, tok, part), bf)
    wide = pltpu.VMEM((nz, 4 * cap, half), bf)
    return pl.pallas_call(
        functools.partial(kernel, cap),
        out_shape=pltpu.VMEM((tok, half), bf),
        in_specs=[hbm] * 6,
        out_specs=vmem,
        scratch_shapes=[
            pltpu.VMEM((tok, half), bf),
            pltpu.VMEM((expert_ids.shape[1], tok), jnp.float32),
            pltpu.VMEM((expert_ids.shape[1], tok), jnp.int32),
            pltpu.VMEM((nz - 1, tok, half), bf), full, full,
            pltpu.VMEM((nz, 4 * cap, width), bf),
            compact, compact, compact, compact,
            pltpu.VMEM((nz, 2 * experts, tok), bf),
            pltpu.VMEM((nz, 2, 16, tok), bf),
            pltpu.VMEM((nz, 2, 16, tok), bf),
            pltpu.VMEM((width, 2 * ff), bf),
            pltpu.VMEM((ff, width), bf),
            pltpu.VMEM((nz, 4 * cap, ff), bf),
            wide, wide, wide, wide,
            compact, compact, compact, compact,
            full, full, full, full,
            pltpu.VMEM((nz - 1, tok, half), bf),
            pltpu.VMEM((nz - 1, tok, half), bf),
            pltpu.VMEM((2, tok, half), bf),
            pltpu.VMEM((nz, 2, tok, part), jnp.float32),
            pltpu.VMEM((tok, half), jnp.float32),
        ],
        compiler_params=pltpu.CompilerParams(
            collective_id=0, has_side_effects=True, vmem_limit_bytes=60 * 1024 * 1024
        ),
    )(tokens, gate_weights.T, expert_ids.T, w_gate, w_up, w_down)


def local(tokens, gate_weights, expert_ids, w_gate, w_up, w_down):
    tok_dev, half = tokens.shape
    devices, cores = lax.axis_size("ep"), lax.axis_size("half")
    experts = w_gate.shape[0] * devices
    cap = slot_count(tok_dev, expert_ids.shape[1], experts)
    fits = tok_dev * devices * half * 2 <= 8 * 1024 * 1024 and w_gate.shape[0] == 1
    shaped = cores == 2 and devices == 4 * 4 and tok_dev == 128
    tiled = cap % 16 == 0 and half % 256 == 0 and experts % 16 == 0 and w_gate.shape[2] % 128 == 0
    plan = multicast if fits and shaped and tiled else slots
    return plan(tokens, gate_weights, expert_ids, w_gate, w_up, w_down)


def solution(mesh):
    placed = (
        P("ep", "half"),
        P("ep", None),
        P("ep", None),
        P("ep", None, "half"),
        P("ep", None, "half"),
        P("ep", "half", None),
    )
    return jax.shard_map(
        local, mesh=mesh, in_specs=placed, out_specs=P("ep", "half"), check_vma=False
    )
```

```python
import functools

import jax
import jax.numpy as jnp
from jax import lax
from jax.experimental import pallas as pl
from jax.experimental.pallas import tpu as pltpu
from jax.sharding import PartitionSpec as P

MESH = pl.DeviceIdType.MESH


def slot_count(tok_dev, top, experts):
    return min(tok_dev, max(2, 5 * tok_dev * top // (4 * experts)))


def slots(tokens, gate_weights, expert_ids, w_gate, w_up, w_down):
    tok_dev, half_width = tokens.shape
    top = expert_ids.shape[1]
    local_experts = w_gate.shape[0]
    experts = local_experts * lax.axis_size("ep")
    capacity = slot_count(tok_dev, top, experts)
    flat_ids = expert_ids.reshape(-1)
    columns = jnp.arange(experts, dtype=jnp.int32)
    onehot = (flat_ids[:, None] == columns[None, :]).astype(jnp.int32)
    ranks = jnp.sum((jnp.cumsum(onehot, axis=0) - onehot) * onehot, axis=1)
    slot = flat_ids * capacity + ranks
    token_of_pair = jnp.arange(tok_dev * top, dtype=jnp.int32) // top
    token_table = jnp.zeros((experts * capacity,), jnp.int32).at[slot].set(token_of_pair)
    filled = (
        jnp.zeros((experts * capacity,), jnp.bfloat16)
        .at[slot]
        .set(jnp.ones((tok_dev * top,), jnp.bfloat16))
    )
    outgoing = (tokens[token_table] * filled[:, None]).reshape(experts, capacity, half_width)
    received = lax.all_to_all(outgoing, "ep", split_axis=0, concat_axis=0, tiled=True)
    count = received.shape[1]
    whole = lax.all_gather(received, "half", axis=2, tiled=True)
    width = whole.shape[2]
    grouped = whole.reshape(-1, local_experts, count, width)
    gate = jnp.einsum("secd,edf->secf", grouped, w_gate, preferred_element_type=jnp.float32)
    up = jnp.einsum("secd,edf->secf", grouped, w_up, preferred_element_type=jnp.float32)
    hidden = (jax.nn.silu(gate) * up).astype(jnp.bfloat16)
    partial_out = jnp.einsum("secf,efd->secd", hidden, w_down, preferred_element_type=jnp.float32)
    partial_out = partial_out.astype(jnp.bfloat16).reshape(experts, count, width)
    widened = lax.optimization_barrier(partial_out).astype(jnp.float32)
    summed = lax.psum_scatter(widened.astype(jnp.bfloat16), "half", scatter_dimension=2, tiled=True)
    answer = lax.all_to_all(summed, "ep", split_axis=0, concat_axis=0, tiled=True)
    picked = answer.reshape(experts * capacity, -1)[slot].reshape(tok_dev, top, -1)
    slot_out = picked.astype(jnp.float32)
    mixed = jnp.einsum("tk,tkx->tx", gate_weights, slot_out)
    return mixed.astype(jnp.bfloat16)


PLANS = (
    (
        "A14", "F0", "G0", "A10", "X0", "Y0", "A11", "A24", "A12", "A13", "T0", "A20", "F1", "U0",
        "G1", "A21", "W", "C0", "A22", "A23", "F2", "G2", "A34", "A30", "D0", "A31", "Y2", "X2",
        "T2", "A32", "A33", "X1", "Y1", "U2", "F3", "G3", "Y3", "X3", "K0", "C2", "D2", "T1", "U1",
        "K2", "T3", "L2", "U3", "C3", "R20", "Q20", "R21", "D3", "K3", "C1", "Q21", "L3", "J20",
        "H20", "D1", "R30", "H21", "R31", "Q30", "J21", "K1", "H30", "Q31", "L1", "J30", "R10",
        "Q10", "H31", "R11", "Q11", "L0", "J31", "H10", "J10", "Q00", "R00", "J11", "R01", "Q01",
        "H11", "J00", "H00", "H01", "J01",
    ),
    (
        "A14", "A24", "A20", "A10", "A21", "A11", "A22", "A12", "A13", "F1", "G1", "A34", "A23",
        "X1", "X0", "A30", "Y1", "A31", "X2", "F2", "A32", "T1", "Y2", "G2", "Y0", "U1", "A33", "W",
        "C1", "F0", "F3", "D1", "U2", "G3", "G0", "T2", "X3", "U0", "Y3", "K1", "C2", "D2", "K2",
        "U3", "T3", "L2", "L1", "Q10", "R20", "Q20", "R21", "Q21", "R10", "C3", "T0", "D3", "K3",
        "C0", "H20", "Q11", "L3", "J20", "H10", "H21", "J10", "M10", "R30", "Q30", "M00", "R11",
        "D0", "J11", "Q31", "J21", "M11", "R31", "H30", "N00", "K0", "L0", "J30", "N10", "H31",
        "J31", "N01", "Q00", "N11", "Q01", "R00", "H11", "R01", "M01", "J00", "H00", "J01", "H01",
    ),
)
MERGE = ((1, 1), (1, 1))


def kernel(cap, *refs):
    dma = pltpu.SemaphoreType.DMA
    pl.run_scoped(functools.partial(body, cap, *refs), dma((12,)), dma((230,)), dma((230,)))


def body(cap, tok_hbm, gw_hbm, ids_hbm, wg_ref, wu_ref, wd_ref, out_ref,
         tok_ref, gw_ref, ids_ref, xo, xa, yb, rows_in, cx, cy, rx, ry, tab, near, seen, wgu, wdn, hid, po, pin, mine, res,
         rda, rdb, rcx, rcy, fx, fy, rfx, rfy, zs, zin, zm, acc, own, load_sem, ssem, rsem):
    ep = lax.axis_index("ep")
    core = lax.axis_index("half")
    x, y, z = ep % 2, (ep // 2) % 2, ep // 4
    tok, half = out_ref.shape
    part, rows, ff = half // 2, tok // 4, wg_ref.shape[2]
    experts = tab.shape[1] // 2
    nz = tab.shape[0]
    f32, bf = jnp.float32, jnp.bfloat16
    inner = ((z + 1) // 2) % 2
    ex, ey, ed = z * 4 + y * 2 + (1 - x), z * 4 + (1 - y) * 2 + x, z * 4 + (1 - y) * 2 + (1 - x)
    other, xn, yn = {"half": 1 - core}, {"ep": ex}, {"ep": ey}
    z1 = {"ep": (z + 1 - 2 * (z % 2)) * 4 + y * 2 + x}
    z3 = {"ep": (nz - 1 - z) * 4 + y * 2 + x}
    left, right = pl.ds(0, part), pl.ds(part, part)
    names = {}

    def send(name, src, dst, to, lands=None):
        at = names.setdefault(name, len(names))
        got = at if lands is None else names.setdefault(lands, len(names))
        return pltpu.make_async_remote_copy(
            src_ref=src, dst_ref=dst, send_sem=ssem.at[at], recv_sem=rsem.at[got],
            device_id=to, device_id_type=MESH,
        )

    sent = []

    def move(copy):
        copy.start()
        sent.append(copy)

    def go(*args):
        move(send(*args))

    barrier = pltpu.get_barrier_semaphore()
    for partner in (other, xn, yn, z1):
        pl.semaphore_signal(barrier, inc=1, device_id=partner, device_id_type=MESH)

    @pl.when(inner == 1)
    def _():
        pl.semaphore_signal(barrier, inc=1, device_id=z3, device_id_type=MESH)

    inputs = [
        pltpu.make_async_copy(src, dst, load_sem.at[6 + at])
        for at, (src, dst) in enumerate(((ids_hbm, ids_ref), (gw_hbm, gw_ref), (tok_hbm, tok_ref)))
    ]
    for load in inputs:
        load.start()
    h0, h1 = pl.ds(core * half, half), pl.ds((1 - core) * half, half)
    loads = []
    for at, (src, cols) in enumerate(((wg_ref, pl.ds(0, ff)), (wu_ref, pl.ds(ff, ff)))):
        for side, deep in enumerate((h0, h1)):
            loads.append(pltpu.make_async_copy(
                src.at[0, deep], wgu.at[pl.ds(side * half, half), cols], load_sem.at[2 * at + side]))
    for side, cols in enumerate((h0, h1)):
        cols = pl.ds(pl.multiple_of(cols.start, 128), half)
        loads.append(pltpu.make_async_copy(
            wd_ref.at[0, :, cols], wdn.at[:, pl.ds(side * half, half)], load_sem.at[4 + side]))
    for load in loads:
        load.start()

    inputs[0].wait()
    inputs[1].wait()
    expert_at = lax.broadcasted_iota(jnp.int32, (experts, tok), 0)
    chosen, weight = jnp.zeros((experts, tok), f32), jnp.zeros((experts, tok), f32)
    for k in range(ids_ref.shape[0]):
        hit = expert_at == ids_ref[k : k + 1, :]
        chosen += jnp.where(hit, 1.0, 0.0)
        weight += jnp.where(hit, gw_ref[k : k + 1, :], 0.0)
    before = lax.broadcasted_iota(jnp.int32, (tok, tok), 0) < lax.broadcasted_iota(jnp.int32, (tok, tok), 1)
    rank = jnp.dot(chosen.astype(bf), jnp.where(before, 1.0, 0.0).astype(bf), preferred_element_type=f32)
    tab[0, 0:experts] = jnp.where(chosen > 0.0, rank, -1.0).astype(bf)
    tab[0, experts : 2 * experts] = weight.astype(bf)

    inputs[2].wait()
    pl.semaphore_wait(barrier, 4 + inner)

    slot_at = lax.broadcasted_iota(jnp.int32, (cap, tok), 0).astype(f32)
    tile_at = lax.broadcasted_iota(jnp.int32, (16, tok), 0)

    def lookup(table, e, base):
        half_of = table[base * experts : (base + 1) * experts].astype(f32)
        return jnp.sum(jnp.where(expert_at == e, half_of, 0.0), axis=0, keepdims=True)

    def row(d, line, who, base):
        if line == 0:
            return lookup(tab[d], {"me": ep, "x": ex, "y": ey}[who], base)
        at = 2 * base + (who != "me")
        return seen[d, line - 1].astype(f32)[at : at + 1]

    def pick(d, line, es):
        parts = [jnp.where(slot_at == row(d, line, e, 0), 1.0, 0.0).astype(bf) for e in es]
        return jnp.concatenate(parts, axis=0)

    def spread(d, line, e, values):
        w = jnp.where(slot_at == row(d, line, e, 0), row(d, line, e, 1), 0.0)
        return lax.dot_general(w.astype(bf), values, (((0,), (0,)), ((), ())), preferred_element_type=f32)

    def block(d):
        return tok_ref if d == 0 else xo.at[d - 1]

    def piece(d, p):
        return tab.at[d] if p == 4 else block(d).at[pl.ds(p * rows, rows)]

    def hop(name, lands, p, came, to):
        return send((name, p), piece(came, p), piece(lands, p), to, ("z", lands, p))

    def plane(d, p):
        if p == 4:
            for line, to, mark in ((1, xn, "xt"), (2, yn, "yt")):
                tile = jnp.zeros((16, tok), f32)
                for at, e in enumerate((ex if line == 1 else ey, ed)):
                    for base in range(2):
                        tile = jnp.where(tile_at == at + 2 * base, lookup(tab[d], e, base), tile)
                near[d, line - 1] = tile.astype(bf)
                go((mark, d), near.at[d, line - 1], seen.at[d, line - 1], to)
        else:
            here = pl.ds(p * rows, rows)
            go(("xf", d, p), block(d).at[here, left], xa.at[d, here], xn)
            go(("yf", d, p), block(d).at[here, right], yb.at[d, here], yn)

    order = (4, 0, 1, 2, 3)

    def begin(role):
        for p in order:
            move(hop("z own", 1 if role else 2, p, 0, z1))
            if role:
                move(hop("z far", 1, p, 0, z3))
            plane(0, p)

    def expect(name, ref):
        send(name, ref, ref, other).wait_recv()

    def arrive(role, d, p):
        expect(("z", d, p), piece(d, p))
        if role:
            lands, to = ((2, z1), (3, z3), (3, z1))[d - 1]
            move(hop("z on" + str(d), lands, p, d, to))
        plane(d, p)

    c1, c2, c3, c4 = (pl.ds(i * cap, cap) for i in range(4))
    lo, hi = pl.ds(0, half), pl.ds(half, half)

    def first_y(d):
        got = jnp.dot(pick(d, 0, ("me", "y")), block(d)[:, left], preferred_element_type=f32).astype(bf)
        rows_in[d, c1, left] = got[:cap]
        cy[d] = got[cap:]
        go(("yc", d), cy.at[d], rows_in.at[d, c3, left], yn)

    def first_x(d):
        got = jnp.dot(pick(d, 0, ("me", "x")), block(d)[:, right], preferred_element_type=f32).astype(bf)
        rows_in[d, c1, right] = got[:cap]
        cx[d] = got[cap:]
        go(("xc", d), cx.at[d], rows_in.at[d, c2, right], xn)
        go(("g1", d), rows_in.at[d, c1, lo], rows_in.at[d, c1, hi], other)

    def cross_x(d):
        expect(("xt", d), seen.at[d, 0])
        for p in range(4):
            expect(("xf", d, p), xa.at[d, pl.ds(p * rows, rows)])
        got = jnp.dot(pick(d, 1, ("me", "y")), xa[d], preferred_element_type=f32).astype(bf)
        rows_in[d, c2, left] = got[:cap]
        ry[d] = got[cap:]
        go(("yr", d), ry.at[d], rows_in.at[d, c4, left], yn)

    def cross_y(d):
        expect(("yt", d), seen.at[d, 1])
        for p in range(4):
            expect(("yf", d, p), yb.at[d, pl.ds(p * rows, rows)])
        got = jnp.dot(pick(d, 2, ("me", "x")), yb[d], preferred_element_type=f32).astype(bf)
        rows_in[d, c3, right] = got[:cap]
        rx[d] = got[cap:]
        go(("xr", d), rx.at[d], rows_in.at[d, c4, right], xn)

    mid = pl.ds(cap, 2 * cap)

    def share_mid(d):
        expect(("xc", d), rows_in.at[d, c2, right])
        expect(("yc", d), rows_in.at[d, c3, left])
        go(("g2", d), rows_in.at[d, mid, lo], rows_in.at[d, mid, hi], other)

    def share_far(d):
        expect(("yr", d), rows_in.at[d, c4, left])
        expect(("xr", d), rows_in.at[d, c4, right])
        go(("g3", d), rows_in.at[d, c4, lo], rows_in.at[d, c4, hi], other)

    def compute(d):
        expect(("g1", d), rows_in.at[d, c1, hi])
        expect(("g2", d), rows_in.at[d, mid, hi])
        expect(("g3", d), rows_in.at[d, c4, hi])
        gu = jnp.dot(rows_in[d], wgu[...], preferred_element_type=f32)
        gate, up = gu[:, :ff], gu[:, ff:]
        hid[d] = (gate / (1.0 + jnp.exp(-gate)) * up).astype(bf)

    rest = pl.ds(0, 3 * cap)
    quarter = part // 2
    bands = {q: pl.ds(q * quarter, quarter) for q in range(2)}

    def project(d):
        po[d] = jnp.dot(hid[d], wdn[:, half:], preferred_element_type=f32).astype(bf)
        go(("pf", d), po.at[d, c4], pin.at[d, c4], other)
        go(("p", d), po.at[d, rest], pin.at[d, rest], other)
        mine[d] = jnp.dot(hid[d], wdn[:, :half], preferred_element_type=f32).astype(bf)

    def close(d):
        expect(("pf", d), pin.at[d, c4])
        res[d, c4] = (mine[d, c4].astype(f32) + pin[d, c4].astype(f32)).astype(bf)
        for q in bands:
            go(("da", d, q), res.at[d, c4, bands[q]], rda.at[d, :, bands[q]], yn)
            go(("db", d, q), res.at[d, c4, pl.ds(part + q * quarter, quarter)], rdb.at[d, :, bands[q]], xn)

    def direct(d):
        expect(("p", d), pin.at[d, rest])
        res[d, rest] = (mine[d, rest].astype(f32) + pin[d, rest].astype(f32)).astype(bf)
        go(("cy", d), res.at[d, c3, left], rcy.at[d], yn)
        go(("cx", d), res.at[d, c2, right], rcx.at[d], xn)

    def relay_x(d, q):
        expect(("da", d, q), rda.at[d, :, bands[q]])
        fx[d, :, bands[q]] = (
            spread(d, 1, "me", res[d, c2, bands[q]]) + spread(d, 1, "y", rda[d, :, bands[q]])
        ).astype(bf)
        go(("fx", d, q), fx.at[d, :, bands[q]], rfx.at[d, :, bands[q]], xn)

    def relay_y(d, q):
        expect(("db", d, q), rdb.at[d, :, bands[q]])
        here = pl.ds(part + q * quarter, quarter)
        fy[d, :, bands[q]] = (
            spread(d, 2, "me", res[d, c3, here]) + spread(d, 2, "x", rdb[d, :, bands[q]])
        ).astype(bf)
        go(("fy", d, q), fy.at[d, :, bands[q]], rfy.at[d, :, bands[q]], yn)

    apart = (z + 1 - 2 * (z % 2), (z + 2) % nz, nz - 1 - z)
    def home(role, p, d, q):
        band, here = bands[q], pl.ds(p * part + q * quarter, quarter)
        e, part_in, full = ("x", rcx, rfy) if p else ("y", rcy, rfx)
        if q == 0:
            expect(("cx" if p else "cy", d), part_in.at[d])
            acc[d, p] = spread(d, 0, "me", res[d, c1, right if p else left]) + spread(d, 0, e, part_in[d])
        expect(("fy" if p else "fx", d, q), full.at[d, :, band])
        total = acc[d, p, :, band] + full[d, :, band].astype(f32)
        if d == 0:
            own[:, here] = total
            return
        zs[d - 1, :, here] = total.astype(bf)
        if role == 0 and d > 1 and MERGE[d - 2][p]:
            go(("o", d, p, q), zs.at[d - 1, :, here], zm.at[d - 2, :, here], z1, ("m", d, p, q))
        elif role == 0 or not ((d == 1 and MERGE[0][p]) or (d == 3 and MERGE[1][p])):
            forward(role, p, d, q)

    def forward(role, p, d, q):
        here = pl.ds(p * part + q * quarter, quarter)
        step = (d + 1) % 3 if role else d - 1
        go(("o", d, p, q), zs.at[d - 1, :, here], zin.at[step, :, here],
           {"ep": apart[step] * 4 + y * 2 + x}, ("s", step, p, q))

    def merge(d, p, q):
        at, here = (0 if d == 1 else 1), pl.ds(p * part + q * quarter, quarter)
        if MERGE[at][p]:
            expect(("m", at + 2, p, q), zm.at[at, :, here])
            zs[d - 1, :, here] = (zs[d - 1, :, here].astype(f32) + zm[at, :, here].astype(f32)).astype(bf)
            forward(1, p, d, q)

    def ready():
        for load in loads:
            load.wait()

    def finish(role):
        for p, cols in enumerate((left, right)):
            total = own[:, cols]
            for step in range(nz - 1):
                if (role == 0 and step == 2 and MERGE[1][p]) or (role == 1 and step == 1 and MERGE[0][p]):
                    continue
                for q in bands:
                    here = pl.ds(p * part + q * quarter, quarter)
                    expect(("s", step, p, q), zin.at[step, :, here])
                total += zin[step, :, cols].astype(f32)
            out_ref[:, cols] = total.astype(bf)
        for copy in sent:
            copy.wait_send()
        sent.clear()

    steps = {
        "F": first_y, "G": first_x, "X": cross_x, "Y": cross_y, "T": share_mid, "U": share_far, "W": ready,
        "C": compute, "D": project, "K": close, "L": direct, "R": relay_x, "Q": relay_y,
        "M": functools.partial(merge, 1), "N": functools.partial(merge, 3),
    }

    def step(role, word):
        at = [int(v) for v in word[1:]]
        if word[0] == "A":
            arrive(role, *at)
        elif word[0] in "HJ":
            home(role, "HJ".index(word[0]), *at)
        else:
            steps[word[0]](*at)

    for role, plan in enumerate(PLANS):
        @pl.when(inner == role)
        def _():
            begin(role)
            for word in plan:
                step(role, word)
            finish(role)


def multicast(tokens, gate_weights, expert_ids, w_gate, w_up, w_down):
    tok, half = tokens.shape
    experts = w_gate.shape[0] * lax.axis_size("ep")
    nz = lax.axis_size("ep") // 4
    part, width, ff = half // 2, w_gate.shape[1], w_gate.shape[2]
    cap = slot_count(tok, expert_ids.shape[1], experts)
    bf = jnp.bfloat16
    vmem, hbm = pl.BlockSpec(memory_space=pltpu.VMEM), pl.BlockSpec(memory_space=pl.ANY)
    compact, full = pltpu.VMEM((nz, cap, part), bf), pltpu.VMEM((nz, tok, part), bf)
    wide = pltpu.VMEM((nz, 4 * cap, half), bf)
    return pl.pallas_call(
        functools.partial(kernel, cap),
        out_shape=pltpu.VMEM((tok, half), bf),
        in_specs=[hbm] * 6,
        out_specs=vmem,
        scratch_shapes=[
            pltpu.VMEM((tok, half), bf),
            pltpu.VMEM((expert_ids.shape[1], tok), jnp.float32),
            pltpu.VMEM((expert_ids.shape[1], tok), jnp.int32),
            pltpu.VMEM((nz - 1, tok, half), bf), full, full,
            pltpu.VMEM((nz, 4 * cap, width), bf),
            compact, compact, compact, compact,
            pltpu.VMEM((nz, 2 * experts, tok), bf),
            pltpu.VMEM((nz, 2, 16, tok), bf),
            pltpu.VMEM((nz, 2, 16, tok), bf),
            pltpu.VMEM((width, 2 * ff), bf),
            pltpu.VMEM((ff, width), bf),
            pltpu.VMEM((nz, 4 * cap, ff), bf),
            wide, wide, wide, wide,
            compact, compact, compact, compact,
            full, full, full, full,
            pltpu.VMEM((nz - 1, tok, half), bf),
            pltpu.VMEM((nz - 1, tok, half), bf),
            pltpu.VMEM((2, tok, half), bf),
            pltpu.VMEM((nz, 2, tok, part), jnp.float32),
            pltpu.VMEM((tok, half), jnp.float32),
        ],
        compiler_params=pltpu.CompilerParams(
            collective_id=0, has_side_effects=True, vmem_limit_bytes=60 * 1024 * 1024
        ),
    )(tokens, gate_weights.T, expert_ids.T, w_gate, w_up, w_down)


def local(tokens, gate_weights, expert_ids, w_gate, w_up, w_down):
    tok_dev, half = tokens.shape
    devices, cores = lax.axis_size("ep"), lax.axis_size("half")
    experts = w_gate.shape[0] * devices
    cap = slot_count(tok_dev, expert_ids.shape[1], experts)
    fits = tok_dev * devices * half * 2 <= 8 * 1024 * 1024 and w_gate.shape[0] == 1
    shaped = cores == 2 and devices == 4 * 4 and tok_dev == 128
    tiled = cap % 16 == 0 and half % 256 == 0 and experts % 16 == 0 and w_gate.shape[2] % 128 == 0
    plan = multicast if fits and shaped and tiled else slots
    return plan(tokens, gate_weights, expert_ids, w_gate, w_up, w_down)


def solution(mesh):
    placed = (
        P("ep", "half"),
        P("ep", None),
        P("ep", None),
        P("ep", None, "half"),
        P("ep", None, "half"),
        P("ep", "half", None),
    )
    return jax.shard_map(
        local, mesh=mesh, in_specs=placed, out_specs=P("ep", "half"), check_vma=False
    )
```

```python
import functools

import jax
import jax.numpy as jnp
from jax import lax
from jax.experimental import pallas as pl
from jax.experimental.pallas import tpu as pltpu
from jax.sharding import PartitionSpec as P

MESH = pl.DeviceIdType.MESH


def slot_count(tok_dev, top, experts):
    return min(tok_dev, max(2, 5 * tok_dev * top // (4 * experts)))


def slots(tokens, gate_weights, expert_ids, w_gate, w_up, w_down):
    tok_dev, half_width = tokens.shape
    top = expert_ids.shape[1]
    local_experts = w_gate.shape[0]
    experts = local_experts * lax.axis_size("ep")
    capacity = slot_count(tok_dev, top, experts)
    flat_ids = expert_ids.reshape(-1)
    columns = jnp.arange(experts, dtype=jnp.int32)
    onehot = (flat_ids[:, None] == columns[None, :]).astype(jnp.int32)
    ranks = jnp.sum((jnp.cumsum(onehot, axis=0) - onehot) * onehot, axis=1)
    slot = flat_ids * capacity + ranks
    token_of_pair = jnp.arange(tok_dev * top, dtype=jnp.int32) // top
    token_table = jnp.zeros((experts * capacity,), jnp.int32).at[slot].set(token_of_pair)
    filled = (
        jnp.zeros((experts * capacity,), jnp.bfloat16)
        .at[slot]
        .set(jnp.ones((tok_dev * top,), jnp.bfloat16))
    )
    outgoing = (tokens[token_table] * filled[:, None]).reshape(experts, capacity, half_width)
    received = lax.all_to_all(outgoing, "ep", split_axis=0, concat_axis=0, tiled=True)
    count = received.shape[1]
    whole = lax.all_gather(received, "half", axis=2, tiled=True)
    width = whole.shape[2]
    grouped = whole.reshape(-1, local_experts, count, width)
    gate = jnp.einsum("secd,edf->secf", grouped, w_gate, preferred_element_type=jnp.float32)
    up = jnp.einsum("secd,edf->secf", grouped, w_up, preferred_element_type=jnp.float32)
    hidden = (jax.nn.silu(gate) * up).astype(jnp.bfloat16)
    partial_out = jnp.einsum("secf,efd->secd", hidden, w_down, preferred_element_type=jnp.float32)
    partial_out = partial_out.astype(jnp.bfloat16).reshape(experts, count, width)
    widened = lax.optimization_barrier(partial_out).astype(jnp.float32)
    summed = lax.psum_scatter(widened.astype(jnp.bfloat16), "half", scatter_dimension=2, tiled=True)
    answer = lax.all_to_all(summed, "ep", split_axis=0, concat_axis=0, tiled=True)
    picked = answer.reshape(experts * capacity, -1)[slot].reshape(tok_dev, top, -1)
    slot_out = picked.astype(jnp.float32)
    mixed = jnp.einsum("tk,tkx->tx", gate_weights, slot_out)
    return mixed.astype(jnp.bfloat16)


PLANS = (
    (
        "F0", "G0", "A14", "A10", "A11", "X0", "A12", "Y0", "A24", "A13", "F1", "T0", "A20", "G1",
        "A21", "A22", "A23", "F2", "G2", "A34", "A30", "Y2", "A31", "X2", "U0", "T2", "A32", "A33",
        "W", "C0", "F3", "G3", "U2", "X3", "Y3", "C2", "X1", "Y1", "D2", "T3", "K2", "U3", "L2",
        "T1", "C3", "U1", "Q20", "R20", "D3", "R21", "Q21", "K3", "C1", "H20", "L3", "D1", "Q30",
        "K1", "H21", "R30", "J20", "D0", "J21", "R31", "Q31", "L1", "J30", "H30", "R10", "R11",
        "K0", "Q10", "Q11", "J31", "H31", "H10", "L0", "H11", "R00", "J10", "R01", "Q00", "J11",
        "Q01", "H00", "J00", "H01", "J01",
    ),
    (
        "F0", "A24", "A14", "G0", "A20", "A10", "A11", "A21", "A22", "A23", "A12", "F2", "A13",
        "A34", "G2", "F1", "A30", "A31", "G1", "Y1", "X1", "A32", "A33", "Y2", "T1", "X2", "U1",
        "F3", "G3", "Y3", "T2", "W", "C1", "Y0", "U2", "X0", "D1", "X3", "T0", "K1", "C2", "L1",
        "D2", "K2", "T3", "Q10", "R10", "U3", "L2", "C3", "D3", "R11", "K3", "U0", "R20", "Q20",
        "L3", "H10", "C0", "J10", "M00", "R21", "Q30", "Q21", "H11", "J20", "R30", "Q31", "M01",
        "D0", "H20", "M10", "K0", "Q11", "H21", "R31", "J30", "N10", "H30", "N00", "L0", "R00",
        "J31", "N11", "H31", "N01", "J21", "R01", "Q00", "J11", "Q01", "M11", "H00", "J00", "J01",
        "H01",
    ),
)
MERGE = ((1, 1), (1, 1))


def kernel(cap, *refs):
    dma = pltpu.SemaphoreType.DMA
    pl.run_scoped(functools.partial(body, cap, *refs), dma((12,)), dma((230,)), dma((230,)))


def body(cap, tok_hbm, gw_hbm, ids_hbm, wg_ref, wu_ref, wd_ref, out_ref,
         tok_ref, gw_ref, ids_ref, xo, xa, yb, rows_in, cx, cy, rx, ry, tab, near, seen, wgu, wdn, hid, po, pin, mine, res,
         rda, rdb, rcx, rcy, fx, fy, rfx, rfy, zs, zin, zm, acc, own, load_sem, ssem, rsem):
    ep = lax.axis_index("ep")
    core = lax.axis_index("half")
    x, y, z = ep % 2, (ep // 2) % 2, ep // 4
    tok, half = out_ref.shape
    part, rows, ff = half // 2, tok // 4, wg_ref.shape[2]
    experts = tab.shape[1] // 2
    nz = tab.shape[0]
    f32, bf = jnp.float32, jnp.bfloat16
    inner = ((z + 1) // 2) % 2
    ex, ey, ed = z * 4 + y * 2 + (1 - x), z * 4 + (1 - y) * 2 + x, z * 4 + (1 - y) * 2 + (1 - x)
    other, xn, yn = {"half": 1 - core}, {"ep": ex}, {"ep": ey}
    z1 = {"ep": (z + 1 - 2 * (z % 2)) * 4 + y * 2 + x}
    z3 = {"ep": (nz - 1 - z) * 4 + y * 2 + x}
    left, right = pl.ds(0, part), pl.ds(part, part)
    names = {}

    def send(name, src, dst, to, lands=None):
        at = names.setdefault(name, len(names))
        got = at if lands is None else names.setdefault(lands, len(names))
        return pltpu.make_async_remote_copy(
            src_ref=src, dst_ref=dst, send_sem=ssem.at[at], recv_sem=rsem.at[got],
            device_id=to, device_id_type=MESH,
        )

    sent = []

    def move(copy):
        copy.start()
        sent.append(copy)

    def go(*args):
        move(send(*args))

    barrier = pltpu.get_barrier_semaphore()
    for partner in (other, xn, yn, z1):
        pl.semaphore_signal(barrier, inc=1, device_id=partner, device_id_type=MESH)

    @pl.when(inner == 1)
    def _():
        pl.semaphore_signal(barrier, inc=1, device_id=z3, device_id_type=MESH)

    inputs = [
        pltpu.make_async_copy(src, dst, load_sem.at[6 + at])
        for at, (src, dst) in enumerate(((ids_hbm, ids_ref), (gw_hbm, gw_ref), (tok_hbm, tok_ref)))
    ]
    for load in inputs:
        load.start()
    h0, h1 = pl.ds(core * half, half), pl.ds((1 - core) * half, half)
    loads = []
    for at, (src, cols) in enumerate(((wg_ref, pl.ds(0, ff)), (wu_ref, pl.ds(ff, ff)))):
        for side, deep in enumerate((h0, h1)):
            loads.append(pltpu.make_async_copy(
                src.at[0, deep], wgu.at[pl.ds(side * half, half), cols], load_sem.at[2 * at + side]))
    for side, cols in enumerate((h0, h1)):
        cols = pl.ds(pl.multiple_of(cols.start, 128), half)
        loads.append(pltpu.make_async_copy(
            wd_ref.at[0, :, cols], wdn.at[:, pl.ds(side * half, half)], load_sem.at[4 + side]))
    for load in loads:
        load.start()

    inputs[0].wait()
    inputs[1].wait()
    expert_at = lax.broadcasted_iota(jnp.int32, (experts, tok), 0)
    chosen, weight = jnp.zeros((experts, tok), f32), jnp.zeros((experts, tok), f32)
    for k in range(ids_ref.shape[0]):
        hit = expert_at == ids_ref[k : k + 1, :]
        chosen += jnp.where(hit, 1.0, 0.0)
        weight += jnp.where(hit, gw_ref[k : k + 1, :], 0.0)
    before = lax.broadcasted_iota(jnp.int32, (tok, tok), 0) < lax.broadcasted_iota(jnp.int32, (tok, tok), 1)
    rank = jnp.dot(chosen.astype(bf), jnp.where(before, 1.0, 0.0).astype(bf), preferred_element_type=f32)
    tab[0, 0:experts] = jnp.where(chosen > 0.0, rank, -1.0).astype(bf)
    tab[0, experts : 2 * experts] = weight.astype(bf)

    inputs[2].wait()
    pl.semaphore_wait(barrier, 4 + inner)

    slot_at = lax.broadcasted_iota(jnp.int32, (cap, tok), 0).astype(f32)
    tile_at = lax.broadcasted_iota(jnp.int32, (16, tok), 0)

    def lookup(table, e, base):
        half_of = table[base * experts : (base + 1) * experts].astype(f32)
        return jnp.sum(jnp.where(expert_at == e, half_of, 0.0), axis=0, keepdims=True)

    def row(d, line, who, base):
        if line == 0:
            return lookup(tab[d], {"me": ep, "x": ex, "y": ey}[who], base)
        at = 2 * base + (who != "me")
        return seen[d, line - 1].astype(f32)[at : at + 1]

    def pick(d, line, es):
        parts = [jnp.where(slot_at == row(d, line, e, 0), 1.0, 0.0).astype(bf) for e in es]
        return jnp.concatenate(parts, axis=0)

    def spread(d, line, e, values):
        w = jnp.where(slot_at == row(d, line, e, 0), row(d, line, e, 1), 0.0)
        return lax.dot_general(w.astype(bf), values, (((0,), (0,)), ((), ())), preferred_element_type=f32)

    def block(d):
        return tok_ref if d == 0 else xo.at[d - 1]

    def piece(d, p):
        return tab.at[d] if p == 4 else block(d).at[pl.ds(p * rows, rows)]

    def hop(name, lands, p, came, to):
        return send((name, p), piece(came, p), piece(lands, p), to, ("z", lands, p))

    def plane(d, p):
        if p == 4:
            for line, to, mark in ((1, xn, "xt"), (2, yn, "yt")):
                tile = jnp.zeros((16, tok), f32)
                for at, e in enumerate((ex if line == 1 else ey, ed)):
                    for base in range(2):
                        tile = jnp.where(tile_at == at + 2 * base, lookup(tab[d], e, base), tile)
                near[d, line - 1] = tile.astype(bf)
                go((mark, d), near.at[d, line - 1], seen.at[d, line - 1], to)
        else:
            here = pl.ds(p * rows, rows)
            go(("xf", d, p), block(d).at[here, left], xa.at[d, here], xn)
            go(("yf", d, p), block(d).at[here, right], yb.at[d, here], yn)

    order = (4, 0, 1, 2, 3)

    def begin(role):
        for p in order:
            move(hop("z own", 1 if role else 2, p, 0, z1))
            if role:
                move(hop("z far", 1, p, 0, z3))
            plane(0, p)

    def expect(name, ref):
        send(name, ref, ref, other).wait_recv()

    def arrive(role, d, p):
        expect(("z", d, p), piece(d, p))
        if role:
            lands, to = ((2, z1), (3, z3), (3, z1))[d - 1]
            move(hop("z on" + str(d), lands, p, d, to))
        plane(d, p)

    c1, c2, c3, c4 = (pl.ds(i * cap, cap) for i in range(4))
    lo, hi = pl.ds(0, half), pl.ds(half, half)

    def first_y(d):
        got = jnp.dot(pick(d, 0, ("me", "y")), block(d)[:, left], preferred_element_type=f32).astype(bf)
        rows_in[d, c1, left] = got[:cap]
        cy[d] = got[cap:]
        go(("yc", d), cy.at[d], rows_in.at[d, c3, left], yn)

    def first_x(d):
        got = jnp.dot(pick(d, 0, ("me", "x")), block(d)[:, right], preferred_element_type=f32).astype(bf)
        rows_in[d, c1, right] = got[:cap]
        cx[d] = got[cap:]
        go(("xc", d), cx.at[d], rows_in.at[d, c2, right], xn)
        go(("g1", d), rows_in.at[d, c1, lo], rows_in.at[d, c1, hi], other)

    def cross_x(d):
        expect(("xt", d), seen.at[d, 0])
        for p in range(4):
            expect(("xf", d, p), xa.at[d, pl.ds(p * rows, rows)])
        got = jnp.dot(pick(d, 1, ("me", "y")), xa[d], preferred_element_type=f32).astype(bf)
        rows_in[d, c2, left] = got[:cap]
        ry[d] = got[cap:]
        go(("yr", d), ry.at[d], rows_in.at[d, c4, left], yn)

    def cross_y(d):
        expect(("yt", d), seen.at[d, 1])
        for p in range(4):
            expect(("yf", d, p), yb.at[d, pl.ds(p * rows, rows)])
        got = jnp.dot(pick(d, 2, ("me", "x")), yb[d], preferred_element_type=f32).astype(bf)
        rows_in[d, c3, right] = got[:cap]
        rx[d] = got[cap:]
        go(("xr", d), rx.at[d], rows_in.at[d, c4, right], xn)

    mid = pl.ds(cap, 2 * cap)

    def share_mid(d):
        expect(("xc", d), rows_in.at[d, c2, right])
        expect(("yc", d), rows_in.at[d, c3, left])
        go(("g2", d), rows_in.at[d, mid, lo], rows_in.at[d, mid, hi], other)

    def share_far(d):
        expect(("yr", d), rows_in.at[d, c4, left])
        expect(("xr", d), rows_in.at[d, c4, right])
        go(("g3", d), rows_in.at[d, c4, lo], rows_in.at[d, c4, hi], other)

    def compute(d):
        expect(("g1", d), rows_in.at[d, c1, hi])
        expect(("g2", d), rows_in.at[d, mid, hi])
        expect(("g3", d), rows_in.at[d, c4, hi])
        gu = jnp.dot(rows_in[d], wgu[...], preferred_element_type=f32)
        gate, up = gu[:, :ff], gu[:, ff:]
        hid[d] = (gate / (1.0 + jnp.exp(-gate)) * up).astype(bf)

    rest = pl.ds(0, 3 * cap)
    quarter = part // 2
    bands = {q: pl.ds(q * quarter, quarter) for q in range(2)}

    def project(d):
        po[d] = jnp.dot(hid[d], wdn[:, half:], preferred_element_type=f32).astype(bf)
        go(("pf", d), po.at[d, c4], pin.at[d, c4], other)
        go(("p", d), po.at[d, rest], pin.at[d, rest], other)
        mine[d] = jnp.dot(hid[d], wdn[:, :half], preferred_element_type=f32).astype(bf)

    def close(d):
        expect(("pf", d), pin.at[d, c4])
        res[d, c4] = (mine[d, c4].astype(f32) + pin[d, c4].astype(f32)).astype(bf)
        for q in bands:
            go(("da", d, q), res.at[d, c4, bands[q]], rda.at[d, :, bands[q]], yn)
            go(("db", d, q), res.at[d, c4, pl.ds(part + q * quarter, quarter)], rdb.at[d, :, bands[q]], xn)

    def direct(d):
        expect(("p", d), pin.at[d, rest])
        res[d, rest] = (mine[d, rest].astype(f32) + pin[d, rest].astype(f32)).astype(bf)
        go(("cy", d), res.at[d, c3, left], rcy.at[d], yn)
        go(("cx", d), res.at[d, c2, right], rcx.at[d], xn)

    def relay_x(d, q):
        ours = spread(d, 1, "me", res[d, c2, bands[q]])
        expect(("da", d, q), rda.at[d, :, bands[q]])
        fx[d, :, bands[q]] = (ours + spread(d, 1, "y", rda[d, :, bands[q]])).astype(bf)
        go(("fx", d, q), fx.at[d, :, bands[q]], rfx.at[d, :, bands[q]], xn)

    def relay_y(d, q):
        ours = spread(d, 2, "me", res[d, c3, pl.ds(part + q * quarter, quarter)])
        expect(("db", d, q), rdb.at[d, :, bands[q]])
        fy[d, :, bands[q]] = (ours + spread(d, 2, "x", rdb[d, :, bands[q]])).astype(bf)
        go(("fy", d, q), fy.at[d, :, bands[q]], rfy.at[d, :, bands[q]], yn)

    apart = (z + 1 - 2 * (z % 2), (z + 2) % nz, nz - 1 - z)
    def home(role, p, d, q):
        band, here = bands[q], pl.ds(p * part + q * quarter, quarter)
        e, part_in, full = ("x", rcx, rfy) if p else ("y", rcy, rfx)
        if q == 0:
            ours = spread(d, 0, "me", res[d, c1, right if p else left])
            expect(("cx" if p else "cy", d), part_in.at[d])
            acc[d, p] = ours + spread(d, 0, e, part_in[d])
        expect(("fy" if p else "fx", d, q), full.at[d, :, band])
        total = acc[d, p, :, band] + full[d, :, band].astype(f32)
        if d == 0:
            own[:, here] = total
            return
        zs[d - 1, :, here] = total.astype(bf)
        if role == 0 and d > 1 and MERGE[d - 2][p]:
            go(("o", d, p, q), zs.at[d - 1, :, here], zm.at[d - 2, :, here], z1, ("m", d, p, q))
        elif role == 0 or not ((d == 1 and MERGE[0][p]) or (d == 3 and MERGE[1][p])):
            forward(role, p, d, q)

    def forward(role, p, d, q):
        here = pl.ds(p * part + q * quarter, quarter)
        step = (d + 1) % 3 if role else d - 1
        go(("o", d, p, q), zs.at[d - 1, :, here], zin.at[step, :, here],
           {"ep": apart[step] * 4 + y * 2 + x}, ("s", step, p, q))

    def merge(d, p, q):
        at, here = (0 if d == 1 else 1), pl.ds(p * part + q * quarter, quarter)
        if MERGE[at][p]:
            expect(("m", at + 2, p, q), zm.at[at, :, here])
            zs[d - 1, :, here] = (zs[d - 1, :, here].astype(f32) + zm[at, :, here].astype(f32)).astype(bf)
            forward(1, p, d, q)

    def ready():
        for load in loads:
            load.wait()

    def finish(role):
        for p, cols in enumerate((left, right)):
            total = own[:, cols]
            for step in range(nz - 1):
                if (role == 0 and step == 2 and MERGE[1][p]) or (role == 1 and step == 1 and MERGE[0][p]):
                    continue
                for q in bands:
                    here = pl.ds(p * part + q * quarter, quarter)
                    expect(("s", step, p, q), zin.at[step, :, here])
                total += zin[step, :, cols].astype(f32)
            out_ref[:, cols] = total.astype(bf)
        for copy in sent:
            copy.wait_send()
        sent.clear()

    steps = {
        "F": first_y, "G": first_x, "X": cross_x, "Y": cross_y, "T": share_mid, "U": share_far, "W": ready,
        "C": compute, "D": project, "K": close, "L": direct, "R": relay_x, "Q": relay_y,
        "M": functools.partial(merge, 1), "N": functools.partial(merge, 3),
    }

    def step(role, word):
        at = [int(v) for v in word[1:]]
        if word[0] == "A":
            arrive(role, *at)
        elif word[0] in "HJ":
            home(role, "HJ".index(word[0]), *at)
        else:
            steps[word[0]](*at)

    for role, plan in enumerate(PLANS):
        @pl.when(inner == role)
        def _():
            begin(role)
            for word in plan:
                step(role, word)
            finish(role)


def multicast(tokens, gate_weights, expert_ids, w_gate, w_up, w_down):
    tok, half = tokens.shape
    experts = w_gate.shape[0] * lax.axis_size("ep")
    nz = lax.axis_size("ep") // 4
    part, width, ff = half // 2, w_gate.shape[1], w_gate.shape[2]
    cap = slot_count(tok, expert_ids.shape[1], experts)
    bf = jnp.bfloat16
    vmem, hbm = pl.BlockSpec(memory_space=pltpu.VMEM), pl.BlockSpec(memory_space=pl.ANY)
    compact, full = pltpu.VMEM((nz, cap, part), bf), pltpu.VMEM((nz, tok, part), bf)
    wide = pltpu.VMEM((nz, 4 * cap, half), bf)
    return pl.pallas_call(
        functools.partial(kernel, cap),
        out_shape=pltpu.VMEM((tok, half), bf),
        in_specs=[hbm] * 6,
        out_specs=vmem,
        scratch_shapes=[
            pltpu.VMEM((tok, half), bf),
            pltpu.VMEM((expert_ids.shape[1], tok), jnp.float32),
            pltpu.VMEM((expert_ids.shape[1], tok), jnp.int32),
            pltpu.VMEM((nz - 1, tok, half), bf), full, full,
            pltpu.VMEM((nz, 4 * cap, width), bf),
            compact, compact, compact, compact,
            pltpu.VMEM((nz, 2 * experts, tok), bf),
            pltpu.VMEM((nz, 2, 16, tok), bf),
            pltpu.VMEM((nz, 2, 16, tok), bf),
            pltpu.VMEM((width, 2 * ff), bf),
            pltpu.VMEM((ff, width), bf),
            pltpu.VMEM((nz, 4 * cap, ff), bf),
            wide, wide, wide, wide,
            compact, compact, compact, compact,
            full, full, full, full,
            pltpu.VMEM((nz - 1, tok, half), bf),
            pltpu.VMEM((nz - 1, tok, half), bf),
            pltpu.VMEM((2, tok, half), bf),
            pltpu.VMEM((nz, 2, tok, part), jnp.float32),
            pltpu.VMEM((tok, half), jnp.float32),
        ],
        compiler_params=pltpu.CompilerParams(
            collective_id=0, has_side_effects=True, vmem_limit_bytes=60 * 1024 * 1024
        ),
    )(tokens, gate_weights.T, expert_ids.T, w_gate, w_up, w_down)


def local(tokens, gate_weights, expert_ids, w_gate, w_up, w_down):
    tok_dev, half = tokens.shape
    devices, cores = lax.axis_size("ep"), lax.axis_size("half")
    experts = w_gate.shape[0] * devices
    cap = slot_count(tok_dev, expert_ids.shape[1], experts)
    fits = tok_dev * devices * half * 2 <= 8 * 1024 * 1024 and w_gate.shape[0] == 1
    shaped = cores == 2 and devices == 4 * 4 and tok_dev == 128
    tiled = cap % 16 == 0 and half % 256 == 0 and experts % 16 == 0 and w_gate.shape[2] % 128 == 0
    plan = multicast if fits and shaped and tiled else slots
    return plan(tokens, gate_weights, expert_ids, w_gate, w_up, w_down)


def solution(mesh):
    placed = (
        P("ep", "half"),
        P("ep", None),
        P("ep", None),
        P("ep", None, "half"),
        P("ep", None, "half"),
        P("ep", "half", None),
    )
    return jax.shard_map(
        local, mesh=mesh, in_specs=placed, out_specs=P("ep", "half"), check_vma=False
    )
```
